16 devices in a mesh: dp: 2 (over y, z), tp: 8 (over x, core).
Axes of the slice: x: 4, y: 2, z: 1, core: 2. Of those that a mesh axis runs over, the one named last changes fastest.
The devices are a block of a 4x4x8 slice.
Arguments:
- x_in: bfloat16 [512, 3584], P(('dp', 'tp')), parts along dimension 0
- w_in: bfloat16 [3584, 18944], P(None, 'tp')
- grad_out: bfloat16 [512, 18944], P('dp', 'tp'), parts along dimension 0
Outputs:
- output 1: bfloat16 [512, 3584], P(('dp', 'tp')), parts along dimension 0
- output 2: float32 [7168, 18944], P('dp', 'tp'), parts along dimension 0
There are 2 independent parts. The reference program is written for one: setup_inputs(seed, part) draws one part's arguments, and reference() takes and returns one part's arrays. A program takes and returns all parts, laid end to end along the dimension named above; an argument that names none is the same for every part.
All inputs are finite; a program needn't handle non-finite values.
Results may differ from the reference program's by a relative error of at most 0.001.
Values are sent between devices in bfloat16 or wider.
A program may use at most 768 MiB of HBM per device.

```python
import jax
import jax.numpy as jnp

TOKENS = 256
HIDDEN = 3584
FFN_DIM = 18944


def setup_inputs(seed: int = 0, part: int = 0) -> dict:
    base_key = jax.random.key(seed)
    part_key = jax.random.fold_in(base_key, part)
    key_x, key_grad = jax.random.split(part_key)
    key_weight = jax.random.key(seed + 1)
    x_in = jax.random.normal(key_x, (TOKENS, HIDDEN), jnp.float32).astype(jnp.bfloat16)
    w_in = (jax.random.normal(key_weight, (HIDDEN, FFN_DIM), jnp.float32) * HIDDEN ** -0.5).astype(jnp.bfloat16)
    grad_scale = (HIDDEN / FFN_DIM) ** 0.5
    grad_out = (jax.random.normal(key_grad, (TOKENS, FFN_DIM), jnp.float32) * grad_scale).astype(jnp.bfloat16)
    return {"x_in": x_in, "w_in": w_in, "grad_out": grad_out}


def reference(x_in, w_in, grad_out):
    grad_x = jnp.dot(grad_out, w_in.T, preferred_element_type=jnp.float32).astype(jnp.bfloat16)
    grad_w = jnp.dot(x_in.T, grad_out, preferred_element_type=jnp.float32)
    return (grad_x, grad_w)
```

```python
import functools

import jax
import jax.numpy as jnp
from jax import lax
from jax.experimental import pallas as pl
from jax.experimental.pallas import tpu as pltpu
from jax.sharding import PartitionSpec as P

MESH = pl.DeviceIdType.MESH
F32 = jnp.float32
BF16 = jnp.bfloat16


def exchange_kernel(n, x_hbm, wt_hbm, gt_hbm, xf_hbm, own_hbm, plus_hbm, minus_hbm,
                    xf, wbuf, gbuf, g, part, rbuf, csum, u1buf,
                    x_sem, g_sem, w_sem, ag_send, ag_recv, pr_send, pr_recv,
                    d_send, d_recv, u_send, u_recv, out_sem):
    rows, width = x_hbm.shape
    half = width // 2
    nb = w_sem.shape[0]
    blk = width // nb
    me = lax.axis_index("tp")
    chips = n // 2
    chip, core = me // 2, lax.rem(me, 2)
    c_right, c_left = lax.rem(chip + 1, chips), lax.rem(chip + chips - 1, chips)
    c_opp = lax.rem(chip + 2, chips)
    right, left, opp = 2 * c_right + core, 2 * c_left + core, 2 * c_opp + core
    peer = 2 * chip + 1 - core

    def at(dev, lo=0, size=None):
        r = pl.ds(pl.multiple_of(dev * rows, rows), rows)
        return xf.at[r, pl.ds(lo, width if size is None else size)]

    own_x = pltpu.make_async_copy(x_hbm, at(me), x_sem)
    own_x.start()
    g_load = pltpu.make_async_copy(gt_hbm, gbuf, g_sem)
    g_load.start()
    seq = [j for p in zip(range(nb // 2), range(nb // 2, nb)) for j in p]
    w_loads = {}
    for j in seq:
        cols = pl.ds(j * blk, blk)
        w_loads[j] = pltpu.make_async_copy(wt_hbm.at[:, cols], wbuf.at[:, cols], w_sem.at[j])
        w_loads[j].start()

    barrier = pltpu.get_barrier_semaphore()
    for dev in (peer, left, right):
        pl.semaphore_signal(barrier, inc=1, device_id={"tp": dev}, device_id_type=MESH)
    pl.semaphore_wait(barrier, 3)

    def send(src, dst, s_sem, r_sem, dev):
        cp = pltpu.make_async_remote_copy(src_ref=src, dst_ref=dst, send_sem=s_sem, recv_sem=r_sem,
                                          device_id={"tp": dev}, device_id_type=MESH)
        cp.start()
        return cp

    own_x.wait()
    ag = {}
    ag[0] = send(at(me, 0, half), at(me, 0, half), ag_send.at[0], ag_recv.at[0], right)
    ag[3] = send(at(me, half, half), at(me, half, half), ag_send.at[3], ag_recv.at[3], left)
    ag[1] = send(at(me, half, half), at(me, half, half), ag_send.at[1], ag_recv.at[1], right)
    ag[2] = send(at(me, 0, half), at(me, 0, half), ag_send.at[2], ag_recv.at[2], left)
    pr = {}
    pr[6] = send(at(me), at(me), pr_send.at[6], pr_recv.at[6], peer)

    def arrived(slot, dev, lo):
        pltpu.make_async_remote_copy(src_ref=at(dev, lo, half), dst_ref=at(dev, lo, half), send_sem=ag_send.at[slot],
                                     recv_sem=ag_recv.at[slot], device_id={"tp": me}, device_id_type=MESH).wait_recv()
        pr[slot] = send(at(dev, lo, half), at(dev, lo, half), pr_send.at[slot], pr_recv.at[slot], peer)

    g_load.wait()
    g[...] = gbuf[...].T

    def partial(j):
        w_loads[j].wait()
        cols = pl.ds(j * blk, blk)
        t = jnp.dot(g[...], wbuf[:, cols], preferred_element_type=F32)
        part[:, :, :, cols] = t.reshape(chips, 2, rows, blk)

    d2d = {}

    def to_peer(j):
        cols = pl.ds(j * blk, blk)
        d2d[j] = send(part.at[:, 1 - core, :, cols], rbuf.at[:, :, cols], d_send.at[j], d_recv.at[j], peer)

    u1 = {}

    def chip_sum(j):
        cols = pl.ds(j * blk, blk)
        d2d[j].wait_recv()
        csum[:, :, cols] = part[:, core, :, cols] + rbuf[:, :, cols]
        u1[j] = send(csum.at[c_opp, :, cols], u1buf.at[:, cols], u_send.at[j], u_recv.at[j],
                     right if j < nb // 2 else left)

    partial(seq[0])
    to_peer(seq[0])
    partial(seq[1])
    to_peer(seq[1])
    chip_sum(seq[0])
    partial(seq[2])
    to_peer(seq[2])
    arrived(0, left, 0)
    ag[4] = send(at(left, 0, half), at(left, 0, half), ag_send.at[4], ag_recv.at[4], right)
    arrived(3, right, half)
    ag[5] = send(at(right, half, half), at(right, half, half), ag_send.at[5], ag_recv.at[5], left)
    chip_sum(seq[1])
    partial(seq[3])
    to_peer(seq[3])
    chip_sum(seq[2])
    arrived(1, left, half)
    arrived(2, right, 0)
    chip_sum(seq[3])

    outs = []

    def out(src, dst):
        cp = pltpu.make_async_copy(src, dst, out_sem.at[len(outs)])
        cp.start()
        outs.append(cp)

    lo, hi = pl.ds(0, half), pl.ds(half, half)
    out(csum.at[chip], own_hbm)
    out(csum.at[c_right, :, hi], plus_hbm.at[:, hi])
    out(csum.at[c_left, :, lo], minus_hbm.at[:, lo])

    arrived(4, opp, 0)
    arrived(5, opp, half)
    for cp in pr.values():
        cp.wait()
    out(xf, xf_hbm)

    for j in seq:
        cols = pl.ds(j * blk, blk)
        u1[j].wait_recv()
        c, dst = (c_right, plus_hbm) if j < nb // 2 else (c_left, minus_hbm)
        csum[c, :, cols] += u1buf[:, cols]
        out(csum.at[c, :, cols], dst.at[:, cols])
    for cp in ag.values():
        cp.wait_send()
    for cp in d2d.values():
        cp.wait_send()
    for cp in u1.values():
        cp.wait_send()
    for cp in outs:
        cp.wait()


def exchange(x_blk, wt_blk, gt_blk, n):
    rows, width = x_blk.shape
    cols, tokens = gt_blk.shape
    chips = n // 2
    nb = 4
    hbm = pl.BlockSpec(memory_space=pltpu.HBM)
    part = jax.ShapeDtypeStruct((rows, width), F32)
    return pl.pallas_call(
        functools.partial(exchange_kernel, n),
        out_shape=(jax.ShapeDtypeStruct((tokens, width), BF16), part, part, part),
        in_specs=[hbm] * 3,
        out_specs=(hbm,) * 4,
        scratch_shapes=[
            pltpu.VMEM((tokens, width), BF16),
            pltpu.VMEM((cols, width), BF16),
            pltpu.VMEM((cols, tokens), BF16),
            pltpu.VMEM((tokens, cols), BF16),
            pltpu.VMEM((chips, 2, rows, width), F32),
            pltpu.VMEM((chips, rows, width), F32),
            pltpu.VMEM((chips, rows, width), F32),
            pltpu.VMEM((rows, width), F32),
            pltpu.SemaphoreType.DMA,
            pltpu.SemaphoreType.DMA,
            pltpu.SemaphoreType.DMA((nb,)),
            pltpu.SemaphoreType.DMA((6,)),
            pltpu.SemaphoreType.DMA((6,)),
            pltpu.SemaphoreType.DMA((7,)),
            pltpu.SemaphoreType.DMA((7,)),
            pltpu.SemaphoreType.DMA((nb,)),
            pltpu.SemaphoreType.DMA((nb,)),
            pltpu.SemaphoreType.DMA((nb,)),
            pltpu.SemaphoreType.DMA((nb,)),
            pltpu.SemaphoreType.DMA((4 + nb,)),
        ],
        compiler_params=pltpu.CompilerParams(collective_id=0, has_side_effects=True, vmem_limit_bytes=60 * 2**20),
        cost_estimate=pl.CostEstimate(flops=2 * tokens * width * cols, bytes_accessed=2 * width * cols,
                                      transcendentals=0),
        name="exchange",
    )(x_blk, wt_blk, gt_blk)


def weight_kernel(x_hbm, gt_hbm, o_hbm, xbuf, gbuf, obuf, x_sem, g_sem, o_sem):
    cols = gbuf.shape[0]
    blk = 256
    starts = [0] + list(range(cols % blk, cols, blk)) if cols % blk else list(range(0, cols, blk))
    ends = starts[1:] + [cols]
    x_load = pltpu.make_async_copy(x_hbm, xbuf, x_sem)
    x_load.start()
    g_load = pltpu.make_async_copy(gt_hbm, gbuf, g_sem)
    g_load.start()
    g_load.wait()
    x_load.wait()
    stores = []
    for i, (a, b) in enumerate(zip(starts, ends)):
        r = pl.ds(a, b - a)
        obuf[r, :] = jnp.dot(gbuf[r, :], xbuf[...], preferred_element_type=F32)
        cp = pltpu.make_async_copy(obuf.at[r, :], o_hbm.at[r, :], o_sem.at[i])
        cp.start()
        stores.append(cp)
    for cp in stores:
        cp.wait()


def weight_grad(x_full, gt_blk):
    tokens, width = x_full.shape
    cols = gt_blk.shape[0]
    hbm = pl.BlockSpec(memory_space=pltpu.HBM)
    return pl.pallas_call(
        weight_kernel,
        out_shape=jax.ShapeDtypeStruct((cols, width), F32),
        in_specs=[hbm] * 2,
        out_specs=hbm,
        scratch_shapes=[
            pltpu.VMEM((tokens, width), BF16),
            pltpu.VMEM((cols, tokens), BF16),
            pltpu.VMEM((cols, width), F32),
            pltpu.SemaphoreType.DMA,
            pltpu.SemaphoreType.DMA,
            pltpu.SemaphoreType.DMA((16,)),
        ],
        compiler_params=pltpu.CompilerParams(vmem_limit_bytes=60 * 2**20),
        cost_estimate=pl.CostEstimate(flops=2 * tokens * width * cols, bytes_accessed=4 * width * cols,
                                      transcendentals=0),
        name="weight_grad",
    )(x_full, gt_blk)


def solution(mesh):
    n = mesh.shape["tp"]

    def per_device(x_blk, w_blk, grad_blk):
        gt_blk = grad_blk.T
        x_full, own, plus, minus = exchange(x_blk, w_blk.T, gt_blk, n)
        from_left = lax.ppermute(plus, "tp", [(i, (i + 2) % n) for i in range(n)])
        from_right = lax.ppermute(minus, "tp", [(i, (i + n - 2) % n) for i in range(n)])
        grad_w = weight_grad(x_full, gt_blk).T
        grad_x = (own + from_left + from_right).astype(BF16)
        return grad_x, grad_w

    return jax.shard_map(
        per_device,
        mesh=mesh,
        in_specs=(P(("dp", "tp"), None), P(None, "tp"), P("dp", "tp")),
        out_specs=(P(("dp", "tp"), None), P("dp", "tp")),
        check_vma=False,
    )
```

```python
import functools

import jax
import jax.numpy as jnp
from jax import lax
from jax.experimental import pallas as pl
from jax.experimental.pallas import tpu as pltpu
from jax.sharding import PartitionSpec as P

MESH = pl.DeviceIdType.MESH
F32 = jnp.float32
BF16 = jnp.bfloat16


def exchange_kernel(n, groups, x_hbm, wt_hbm, gt_hbm, xf, gt, own, plus, minus,
                    wbuf, g, part, rbuf, opp_sum, u1buf,
                    x_sem, g_sem, w_sem, ag_send, ag_recv, pr_send, pr_recv,
                    d_send, d_recv, u_send, u_recv):
    rows, width = x_hbm.shape
    half = rows // 2
    nb = w_sem.shape[0]
    blk = width // nb
    me = lax.axis_index("tp")
    chips = n // 2
    chip, core = me // 2, lax.rem(me, 2)
    c_right, c_left = lax.rem(chip + 1, chips), lax.rem(chip + chips - 1, chips)
    c_opp = lax.rem(chip + 2, chips)
    right, left, opp = 2 * c_right + core, 2 * c_left + core, 2 * c_opp + core
    peer = 2 * chip + 1 - core
    lo, hi = pl.ds(0, half), pl.ds(half, half)

    def at(dev, part_of=0, size=rows):
        return xf.at[pl.ds(pl.multiple_of(dev * rows + part_of * half, half), size), :]

    def low(dev):
        return at(dev, 0, half)

    def high(dev):
        return at(dev, 1, half)

    own_x = pltpu.make_async_copy(x_hbm, at(me), x_sem)
    own_x.start()
    g_load = pltpu.make_async_copy(gt_hbm, gt, g_sem)
    g_load.start()
    ahead = 3

    def w_load(j):
        cols = pl.ds(j * blk, blk)
        return pltpu.make_async_copy(wt_hbm.at[:, cols], wbuf.at[:, cols], w_sem.at[j])

    for j in range(ahead):
        w_load(j).start()

    barrier = pltpu.get_barrier_semaphore()
    for dev in (left, right, peer):
        pl.semaphore_signal(barrier, inc=1, device_id={"tp": dev}, device_id_type=MESH)
    pl.semaphore_wait(barrier, 3)

    def send(src, dst, s_sem, r_sem, dev):
        cp = pltpu.make_async_remote_copy(src_ref=src, dst_ref=dst, send_sem=s_sem, recv_sem=r_sem,
                                          device_id={"tp": dev}, device_id_type=MESH)
        cp.start()
        return cp

    own_x.wait()
    ag = {}
    ag[0] = send(low(me), low(me), ag_send.at[0], ag_recv.at[0], right)
    ag[3] = send(high(me), high(me), ag_send.at[3], ag_recv.at[3], left)
    ag[1] = send(high(me), high(me), ag_send.at[1], ag_recv.at[1], right)
    ag[2] = send(low(me), low(me), ag_send.at[2], ag_recv.at[2], left)
    pr = {}
    pr[6] = send(at(me), at(me), pr_send.at[6], pr_recv.at[6], peer)

    def arrived(slot, block, onward=None):
        pltpu.make_async_remote_copy(src_ref=block, dst_ref=block, send_sem=ag_send.at[slot],
                                     recv_sem=ag_recv.at[slot], device_id={"tp": me}, device_id_type=MESH).wait_recv()
        if onward is not None:
            to, dev = onward
            ag[to] = send(block, block, ag_send.at[to], ag_recv.at[to], dev)
        pr[slot] = send(block, block, pr_send.at[slot], pr_recv.at[slot], peer)

    g_load.wait()
    g[...] = gt[...].T

    d2d = {}

    def partial(j):
        w_load(j).wait()
        if j + ahead < nb:
            w_load(j + ahead).start()
        cols = pl.ds(j * blk, blk)
        t = jnp.dot(g[...], wbuf[:, cols], preferred_element_type=F32)
        part[:, :, :, cols] = t.reshape(chips, 2, rows, blk)
        d2d[j] = send(part.at[:, 1 - core, :, cols], rbuf.at[:, :, cols], d_send.at[j], d_recv.at[j], peer)

    u1 = []

    def chip_sum(js):
        for j in js:
            cols = pl.ds(j * blk, blk)
            d2d[j].wait_recv()
            opp_sum[:, cols] = part[c_opp, core, :, cols] + rbuf[c_opp, :, cols]
            own[:, cols] = part[chip, core, :, cols] + rbuf[chip, :, cols]
            plus[:, cols] = part[c_right, core, :, cols] + rbuf[c_right, :, cols]
            minus[:, cols] = part[c_left, core, :, cols] + rbuf[c_left, :, cols]
        cols = pl.ds(js[0] * blk, len(js) * blk)
        k = len(u1)
        u1.append((js, send(opp_sum.at[lo, cols], u1buf.at[lo, cols], u_send.at[0, k], u_recv.at[0, k], right),
                   send(opp_sum.at[hi, cols], u1buf.at[hi, cols], u_send.at[1, k], u_recv.at[1, k], left)))

    for j in range(4):
        partial(j)
    arrived(0, low(left), (4, right))
    arrived(3, high(right), (5, left))
    chip_sum(groups[0])
    partial(4)
    arrived(1, high(left))
    arrived(2, low(right))
    partial(5)
    partial(6)
    chip_sum(groups[1])
    chip_sum(groups[2])
    arrived(4, low(opp))
    arrived(5, high(opp))
    for js, from_left, from_right in u1:
        cols = pl.ds(js[0] * blk, len(js) * blk)
        from_left.wait_recv()
        plus[lo, cols] += u1buf[lo, cols]
        from_right.wait_recv()
        minus[hi, cols] += u1buf[hi, cols]
    for cp in pr.values():
        cp.wait()
    for cp in ag.values():
        cp.wait_send()
    for cp in d2d.values():
        cp.wait_send()
    for _, a, b in u1:
        a.wait_send()
        b.wait_send()


def exchange(x_blk, wt_blk, gt_blk, n):
    rows, width = x_blk.shape
    cols, tokens = gt_blk.shape
    chips = n // 2
    nb = 7
    groups = ((0, 1, 2, 3), (4, 5), (6,))
    hbm = pl.BlockSpec(memory_space=pltpu.HBM)
    vmem = pl.BlockSpec(memory_space=pltpu.VMEM)
    part = pltpu.VMEM((rows, width), F32)
    return pl.pallas_call(
        functools.partial(exchange_kernel, n, groups),
        out_shape=(pltpu.VMEM((tokens, width), BF16), pltpu.VMEM((cols, tokens), BF16), part, part, part),
        in_specs=[hbm] * 3,
        out_specs=(vmem,) * 5,
        scratch_shapes=[
            pltpu.VMEM((cols, width), BF16),
            pltpu.VMEM((tokens, cols), BF16),
            pltpu.VMEM((chips, 2, rows, width), F32),
            pltpu.VMEM((chips, rows, width), F32),
            pltpu.VMEM((rows, width), F32),
            pltpu.VMEM((rows, width), F32),
            pltpu.SemaphoreType.DMA,
            pltpu.SemaphoreType.DMA,
            pltpu.SemaphoreType.DMA((nb,)),
            pltpu.SemaphoreType.DMA((6,)),
            pltpu.SemaphoreType.DMA((6,)),
            pltpu.SemaphoreType.DMA((7,)),
            pltpu.SemaphoreType.DMA((7,)),
            pltpu.SemaphoreType.DMA((nb,)),
            pltpu.SemaphoreType.DMA((nb,)),
            pltpu.SemaphoreType.DMA((2, len(groups))),
            pltpu.SemaphoreType.DMA((2, len(groups))),
        ],
        compiler_params=pltpu.CompilerParams(collective_id=0, has_side_effects=True, vmem_limit_bytes=32 * 2**20),
        cost_estimate=pl.CostEstimate(flops=2 * tokens * width * cols, bytes_accessed=2 * width * cols,
                                      transcendentals=0),
        name="exchange",
    )(*(pltpu.with_memory_space_constraint(a, pltpu.HBM) for a in (x_blk, wt_blk, gt_blk)))


def weight_kernel(x, gt, o_hbm, obuf, o_sem):
    cols = gt.shape[0]
    blk = 256
    starts = ([0] if cols % blk else []) + list(range(cols % blk, cols, blk))
    ends = starts[1:] + [cols]
    stores = []
    for i, (a, b) in enumerate(zip(starts, ends)):
        r = pl.ds(a, b - a)
        obuf[r, :] = jnp.dot(gt[r, :], x[...], preferred_element_type=F32)
        cp = pltpu.make_async_copy(obuf.at[r, :], o_hbm.at[r, :], o_sem.at[i])
        cp.start()
        stores.append(cp)
    for cp in stores:
        cp.wait()


def weight_grad(x_full, gt_blk):
    tokens, width = x_full.shape
    cols = gt_blk.shape[0]
    vmem = pl.BlockSpec(memory_space=pltpu.VMEM)
    return pl.pallas_call(
        weight_kernel,
        out_shape=jax.ShapeDtypeStruct((cols, width), F32),
        in_specs=[vmem] * 2,
        out_specs=pl.BlockSpec(memory_space=pltpu.HBM),
        scratch_shapes=[pltpu.VMEM((cols, width), F32), pltpu.SemaphoreType.DMA((16,))],
        compiler_params=pltpu.CompilerParams(vmem_limit_bytes=40 * 2**20),
        cost_estimate=pl.CostEstimate(flops=2 * tokens * width * cols, bytes_accessed=4 * width * cols,
                                      transcendentals=0),
        name="weight_grad",
    )(x_full, gt_blk)


def solution(mesh):
    n = mesh.shape["tp"]

    def per_device(x_blk, w_blk, grad_blk):
        x_full, gt_blk, own, plus, minus = exchange(x_blk, w_blk.T, grad_blk.T, n)
        from_left = lax.ppermute(plus, "tp", [(i, (i + 2) % n) for i in range(n)])
        from_right = lax.ppermute(minus, "tp", [(i, (i + n - 2) % n) for i in range(n)])
        grad_w = weight_grad(x_full, gt_blk).T
        grad_x = (own + from_left + from_right).astype(BF16)
        return grad_x, grad_w

    return jax.shard_map(
        per_device,
        mesh=mesh,
        in_specs=(P(("dp", "tp"), None), P(None, "tp"), P("dp", "tp")),
        out_specs=(P(("dp", "tp"), None), P("dp", "tp")),
        check_vma=False,
    )
```

```python
import functools

import jax
import jax.numpy as jnp
from jax import lax
from jax.experimental import pallas as pl
from jax.experimental.pallas import tpu as pltpu
from jax.sharding import PartitionSpec as P

MESH = pl.DeviceIdType.MESH
F32 = jnp.float32
BF16 = jnp.bfloat16


def exchange_kernel(n, x_hbm, wt_hbm, gt_hbm, xf, gt, own, plus, minus,
                    wbuf, g, part, rbuf, opp_sum, u1buf,
                    x_sem, g_sem, w_sem, ag_send, ag_recv, pr_send, pr_recv,
                    d_send, d_recv, u_send, u_recv):
    rows, width = x_hbm.shape
    half = rows // 2
    nb = w_sem.shape[0]
    blk = width // nb
    me = lax.axis_index("tp")
    chips = n // 2
    chip, core = me // 2, lax.rem(me, 2)
    c_right, c_left = lax.rem(chip + 1, chips), lax.rem(chip + chips - 1, chips)
    c_opp = lax.rem(chip + 2, chips)
    right, left, opp = 2 * c_right + core, 2 * c_left + core, 2 * c_opp + core
    peer = 2 * chip + 1 - core
    lo, hi = pl.ds(0, half), pl.ds(half, half)

    def at(dev, part_of=0, size=rows):
        return xf.at[pl.ds(pl.multiple_of(dev * rows + part_of * half, half), size), :]

    def low(dev):
        return at(dev, 0, half)

    def high(dev):
        return at(dev, 1, half)

    own_x = pltpu.make_async_copy(x_hbm, at(me), x_sem)
    own_x.start()
    g_load = pltpu.make_async_copy(gt_hbm, gt, g_sem)
    g_load.start()
    ahead = 4

    def w_load(j):
        cols = pl.ds(pl.multiple_of(j * blk, blk), blk)
        return pltpu.make_async_copy(wt_hbm.at[:, cols], wbuf.at[:, cols], w_sem.at[j])

    for j in range(ahead):
        w_load(j).start()

    barrier = pltpu.get_barrier_semaphore()
    for dev in (left, right, peer):
        pl.semaphore_signal(barrier, inc=1, device_id={"tp": dev}, device_id_type=MESH)
    pl.semaphore_wait(barrier, 3)

    def remote(src, dst, s_sem, r_sem, dev):
        return pltpu.make_async_remote_copy(src_ref=src, dst_ref=dst, send_sem=s_sem, recv_sem=r_sem,
                                            device_id={"tp": dev}, device_id_type=MESH)

    def gather(slot, src, dev):
        remote(src, src, ag_send.at[slot], ag_recv.at[slot], dev).start()

    def relay(slot, src):
        return remote(src, src, pr_send.at[slot], pr_recv.at[slot], peer)

    own_x.wait()
    gather(0, low(me), right)
    gather(3, high(me), left)
    gather(1, high(me), right)
    gather(2, low(me), left)
    relay(6, at(me)).start()

    def arrived(slot, src, onward=None):
        remote(src, src, ag_send.at[slot], ag_recv.at[slot], me).wait_recv()
        if onward is not None:
            gather(onward[0], src, onward[1])
        relay(slot, src).start()

    g_load.wait()
    g[...] = gt[...].T

    def block(j):
        return pl.ds(pl.multiple_of(j * blk, blk), blk)

    def to_peer(j):
        return pltpu.make_async_remote_copy(
            src_ref=part.at[:, 1 - core, :, block(j)], dst_ref=rbuf.at[:, :, block(j)],
            send_sem=d_send.at[j], recv_sem=d_recv.at[j], device_id={"tp": peer}, device_id_type=MESH)

    def onward(j, side, dev):
        src = opp_sum.at[side, block(j)]
        k = 0 if side is lo else 1
        return pltpu.make_async_remote_copy(
            src_ref=src, dst_ref=u1buf.at[side, block(j)], send_sem=u_send.at[k, j], recv_sem=u_recv.at[k, j],
            device_id={"tp": dev}, device_id_type=MESH)

    def chip_sum(j):
        to_peer(j).wait_recv()
        cols = block(j)
        opp_sum[:, cols] = part[c_opp, core, :, cols] + rbuf[c_opp, :, cols]
        own[:, cols] = part[chip, core, :, cols] + rbuf[chip, :, cols]
        plus[:, cols] = part[c_right, core, :, cols] + rbuf[c_right, :, cols]
        minus[:, cols] = part[c_left, core, :, cols] + rbuf[c_left, :, cols]
        onward(j, lo, right).start()
        onward(j, hi, left).start()

    lag = 3

    def step(j, carry):
        w_load(j).wait()

        @pl.when(j + ahead < nb)
        def _():
            w_load(j + ahead).start()

        t = jnp.dot(g[...], wbuf[:, block(j)], preferred_element_type=F32)
        part[:, :, :, block(j)] = t.reshape(chips, 2, rows, blk)
        to_peer(j).start()

        @pl.when(j == lag)
        def _():
            arrived(0, low(left), (4, right))
            arrived(3, high(right), (5, left))

        @pl.when(j == lag + 1)
        def _():
            arrived(1, high(left))
            arrived(2, low(right))

        @pl.when(j >= lag)
        def _():
            chip_sum(j - lag)

        return carry

    def each(first, last, f):
        def body(j, carry):
            f(j)
            return carry

        lax.fori_loop(first, last, body, 0)

    lax.fori_loop(0, nb, step, 0)
    each(nb - lag, nb, chip_sum)
    arrived(4, low(opp))
    arrived(5, high(opp))

    def finish(j):
        onward(j, lo, right).wait_recv()
        plus[lo, block(j)] += u1buf[lo, block(j)]
        onward(j, hi, left).wait_recv()
        minus[hi, block(j)] += u1buf[hi, block(j)]

    each(0, nb, finish)
    for slot, block_x in ((0, low(left)), (1, high(left)), (2, low(right)), (3, high(right)), (4, low(opp)),
                          (5, high(opp)), (6, at(me))):
        relay(slot, block_x).wait()
        if slot < 6:
            remote(block_x, block_x, ag_send.at[slot], ag_recv.at[slot], me).wait_send()

    def drain(j):
        to_peer(j).wait_send()
        onward(j, lo, right).wait_send()
        onward(j, hi, left).wait_send()

    each(0, nb, drain)


def exchange(x_blk, wt_blk, gt_blk, n):
    rows, width = x_blk.shape
    cols, tokens = gt_blk.shape
    chips = n // 2
    nb = 7
    hbm = pl.BlockSpec(memory_space=pltpu.HBM)
    vmem = pl.BlockSpec(memory_space=pltpu.VMEM)
    part = pltpu.VMEM((rows, width), F32)
    return pl.pallas_call(
        functools.partial(exchange_kernel, n),
        out_shape=(pltpu.VMEM((tokens, width), BF16), pltpu.VMEM((cols, tokens), BF16), part, part, part),
        in_specs=[hbm] * 3,
        out_specs=(vmem,) * 5,
        scratch_shapes=[
            pltpu.VMEM((cols, width), BF16),
            pltpu.VMEM((tokens, cols), BF16),
            pltpu.VMEM((chips, 2, rows, width), F32),
            pltpu.VMEM((chips, rows, width), F32),
            pltpu.VMEM((rows, width), F32),
            pltpu.VMEM((rows, width), F32),
            pltpu.SemaphoreType.DMA,
            pltpu.SemaphoreType.DMA,
            pltpu.SemaphoreType.DMA((nb,)),
            pltpu.SemaphoreType.DMA((6,)),
            pltpu.SemaphoreType.DMA((6,)),
            pltpu.SemaphoreType.DMA((7,)),
            pltpu.SemaphoreType.DMA((7,)),
            pltpu.SemaphoreType.DMA((nb,)),
            pltpu.SemaphoreType.DMA((nb,)),
            pltpu.SemaphoreType.DMA((2, nb)),
            pltpu.SemaphoreType.DMA((2, nb)),
        ],
        compiler_params=pltpu.CompilerParams(collective_id=0, has_side_effects=True, vmem_limit_bytes=32 * 2**20),
        cost_estimate=pl.CostEstimate(flops=2 * tokens * width * cols, bytes_accessed=2 * width * cols,
                                      transcendentals=0),
        name="exchange",
    )(*(pltpu.with_memory_space_constraint(a, pltpu.HBM) for a in (x_blk, wt_blk, gt_blk)))


def weight_kernel(x, gt, o_hbm, obuf, o_sem):
    cols = gt.shape[0]
    blk = 256
    rest = cols % blk

    def store(start, size, sem):
        return pltpu.make_async_copy(obuf.at[pl.ds(start, size), :], o_hbm.at[pl.ds(start, size), :], sem)

    def rows_of(start, size, sem):
        obuf[pl.ds(start, size), :] = jnp.dot(gt[pl.ds(start, size), :], x[...], preferred_element_type=F32)
        store(start, size, sem).start()

    def at(i):
        return pl.multiple_of(rest + i * blk, 64)

    if rest:
        rows_of(0, rest, o_sem.at[cols // blk])

    def step(i, carry):
        rows_of(at(i), blk, o_sem.at[i])
        return carry

    def drain(i, carry):
        store(at(i), blk, o_sem.at[i]).wait()
        return carry

    lax.fori_loop(0, cols // blk, step, 0)
    lax.fori_loop(0, cols // blk, drain, 0)
    if rest:
        store(0, rest, o_sem.at[cols // blk]).wait()


def weight_grad(x_full, gt_blk):
    tokens, width = x_full.shape
    cols = gt_blk.shape[0]
    vmem = pl.BlockSpec(memory_space=pltpu.VMEM)
    return pl.pallas_call(
        weight_kernel,
        out_shape=jax.ShapeDtypeStruct((cols, width), F32),
        in_specs=[vmem] * 2,
        out_specs=pl.BlockSpec(memory_space=pltpu.HBM),
        scratch_shapes=[pltpu.VMEM((cols, width), F32), pltpu.SemaphoreType.DMA((cols // 256 + 1,))],
        compiler_params=pltpu.CompilerParams(vmem_limit_bytes=40 * 2**20),
        cost_estimate=pl.CostEstimate(flops=2 * tokens * width * cols, bytes_accessed=4 * width * cols,
                                      transcendentals=0),
        name="weight_grad",
    )(x_full, gt_blk)


def solution(mesh):
    n = mesh.shape["tp"]

    def per_device(x_blk, w_blk, grad_blk):
        x_full, gt_blk, own, plus, minus = exchange(x_blk, w_blk.T, grad_blk.T, n)
        from_left = lax.ppermute(plus, "tp", [(i, (i + 2) % n) for i in range(n)])
        from_right = lax.ppermute(minus, "tp", [(i, (i + n - 2) % n) for i in range(n)])
        grad_w = weight_grad(x_full, gt_blk).T
        grad_x = (own + from_left + from_right).astype(BF16)
        return grad_x, grad_w

    return jax.shard_map(
        per_device,
        mesh=mesh,
        in_specs=(P(("dp", "tp"), None), P(None, "tp"), P("dp", "tp")),
        out_specs=(P(("dp", "tp"), None), P("dp", "tp")),
        check_vma=False,
    )
```

```python
import functools

import jax
import jax.numpy as jnp
from jax import lax
from jax.experimental import pallas as pl
from jax.experimental.pallas import tpu as pltpu
from jax.sharding import PartitionSpec as P

MESH = pl.DeviceIdType.MESH
F32 = jnp.float32
BF16 = jnp.bfloat16


def exchange_kernel(n, groups, x_hbm, wt_hbm, gt_hbm, xf, gt, own, plus, minus,
                    wbuf, g, part, rbuf, opp_sum, u1buf,
                    x_sem, g_sem, w_sem, ag_send, ag_recv, pr_send, pr_recv,
                    d_send, d_recv, u_send, u_recv):
    rows, width = x_hbm.shape
    half = rows // 2
    nb = w_sem.shape[0]
    blk = width // nb
    me = lax.axis_index("tp")
    chips = n // 2
    chip, core = me // 2, lax.rem(me, 2)
    c_right, c_left = lax.rem(chip + 1, chips), lax.rem(chip + chips - 1, chips)
    c_opp = lax.rem(chip + 2, chips)
    right, left, opp = 2 * c_right + core, 2 * c_left + core, 2 * c_opp + core
    peer = 2 * chip + 1 - core
    lo, hi = pl.ds(0, half), pl.ds(half, half)

    def at(dev, part_of=0, size=rows):
        return xf.at[pl.ds(pl.multiple_of(dev * rows + part_of * half, half), size), :]

    def low(dev):
        return at(dev, 0, half)

    def high(dev):
        return at(dev, 1, half)

    own_x = pltpu.make_async_copy(x_hbm, at(me), x_sem)
    own_x.start()
    g_load = pltpu.make_async_copy(gt_hbm, gt, g_sem)
    g_load.start()
    ahead = 3

    def w_load(j):
        cols = pl.ds(j * blk, blk)
        return pltpu.make_async_copy(wt_hbm.at[:, cols], wbuf.at[:, cols], w_sem.at[j])

    for j in range(ahead):
        w_load(j).start()

    barrier = pltpu.get_barrier_semaphore()
    for dev in (left, right, peer):
        pl.semaphore_signal(barrier, inc=1, device_id={"tp": dev}, device_id_type=MESH)
    pl.semaphore_wait(barrier, 3)

    def send(src, dst, s_sem, r_sem, dev):
        cp = pltpu.make_async_remote_copy(src_ref=src, dst_ref=dst, send_sem=s_sem, recv_sem=r_sem,
                                          device_id={"tp": dev}, device_id_type=MESH)
        cp.start()
        return cp

    own_x.wait()
    ag = {}
    ag[0] = send(low(me), low(me), ag_send.at[0], ag_recv.at[0], right)
    ag[3] = send(high(me), high(me), ag_send.at[3], ag_recv.at[3], left)
    ag[1] = send(high(me), high(me), ag_send.at[1], ag_recv.at[1], right)
    ag[2] = send(low(me), low(me), ag_send.at[2], ag_recv.at[2], left)
    pr = {}
    pr[6] = send(at(me), at(me), pr_send.at[6], pr_recv.at[6], peer)

    def arrived(slot, block, onward=None):
        pltpu.make_async_remote_copy(src_ref=block, dst_ref=block, send_sem=ag_send.at[slot],
                                     recv_sem=ag_recv.at[slot], device_id={"tp": me}, device_id_type=MESH).wait_recv()
        if onward is not None:
            to, dev = onward
            ag[to] = send(block, block, ag_send.at[to], ag_recv.at[to], dev)
        pr[slot] = send(block, block, pr_send.at[slot], pr_recv.at[slot], peer)

    g_load.wait()
    g[...] = gt[...].T

    d2d = {}

    def partial(j):
        w_load(j).wait()
        if j + ahead < nb:
            w_load(j + ahead).start()
        cols = pl.ds(j * blk, blk)
        t = jnp.dot(g[...], wbuf[:, cols], preferred_element_type=F32)
        t = t.reshape(chips, 2, rows, blk)
        for c in range(2):
            part[j, c] = t[:, c]
        d2d[j] = send(part.at[j, 1 - core], rbuf.at[j], d_send.at[j], d_recv.at[j], peer)

    u1 = []

    def chip_sum(js):
        for j in js:
            cols = pl.ds(j * blk, blk)
            d2d[j].wait_recv()
            opp_sum[j] = part[j, core, c_opp] + rbuf[j, c_opp]
            own[:, cols] = part[j, core, chip] + rbuf[j, chip]
            plus[:, cols] = part[j, core, c_right] + rbuf[j, c_right]
            minus[:, cols] = part[j, core, c_left] + rbuf[j, c_left]
        g0 = pl.ds(js[0], len(js))
        k = len(u1)
        u1.append((js, send(opp_sum.at[g0, lo], u1buf.at[g0, lo], u_send.at[0, k], u_recv.at[0, k], right),
                   send(opp_sum.at[g0, hi], u1buf.at[g0, hi], u_send.at[1, k], u_recv.at[1, k], left)))

    for j in range(4):
        partial(j)
    arrived(0, low(left), (4, right))
    arrived(3, high(right), (5, left))
    chip_sum(groups[0])
    partial(4)
    arrived(1, high(left))
    arrived(2, low(right))
    partial(5)
    partial(6)
    chip_sum(groups[1])
    chip_sum(groups[2])
    arrived(4, low(opp))
    arrived(5, high(opp))
    for js, from_left, from_right in u1:
        from_left.wait_recv()
        from_right.wait_recv()
        for j in js:
            cols = pl.ds(j * blk, blk)
            plus[lo, cols] += u1buf[j, lo]
            minus[hi, cols] += u1buf[j, hi]
    for cp in pr.values():
        cp.wait()
    for cp in ag.values():
        cp.wait_send()
    for cp in d2d.values():
        cp.wait_send()
    for _, a, b in u1:
        a.wait_send()
        b.wait_send()


def exchange(x_blk, wt_blk, gt_blk, n):
    rows, width = x_blk.shape
    cols, tokens = gt_blk.shape
    chips = n // 2
    nb = 7
    groups = ((0, 1, 2, 3), (4, 5), (6,))
    hbm = pl.BlockSpec(memory_space=pltpu.HBM)
    vmem = pl.BlockSpec(memory_space=pltpu.VMEM)
    part = pltpu.VMEM((rows, width), F32)
    return pl.pallas_call(
        functools.partial(exchange_kernel, n, groups),
        out_shape=(pltpu.VMEM((tokens, width), BF16), pltpu.VMEM((cols, tokens), BF16), part, part, part),
        in_specs=[hbm] * 3,
        out_specs=(vmem,) * 5,
        scratch_shapes=[
            pltpu.VMEM((cols, width), BF16),
            pltpu.VMEM((tokens, cols), BF16),
            pltpu.VMEM((nb, 2, chips, rows, width // nb), F32),
            pltpu.VMEM((nb, chips, rows, width // nb), F32),
            pltpu.VMEM((nb, rows, width // nb), F32),
            pltpu.VMEM((nb, rows, width // nb), F32),
            pltpu.SemaphoreType.DMA,
            pltpu.SemaphoreType.DMA,
            pltpu.SemaphoreType.DMA((nb,)),
            pltpu.SemaphoreType.DMA((6,)),
            pltpu.SemaphoreType.DMA((6,)),
            pltpu.SemaphoreType.DMA((7,)),
            pltpu.SemaphoreType.DMA((7,)),
            pltpu.SemaphoreType.DMA((nb,)),
            pltpu.SemaphoreType.DMA((nb,)),
            pltpu.SemaphoreType.DMA((2, len(groups))),
            pltpu.SemaphoreType.DMA((2, len(groups))),
        ],
        compiler_params=pltpu.CompilerParams(collective_id=0, has_side_effects=True, vmem_limit_bytes=32 * 2**20),
        cost_estimate=pl.CostEstimate(flops=2 * tokens * width * cols, bytes_accessed=2 * width * cols,
                                      transcendentals=0),
        name="exchange",
    )(*(pltpu.with_memory_space_constraint(a, pltpu.HBM) for a in (x_blk, wt_blk, gt_blk)))


def weight_kernel(x, gt, o_hbm, obuf, o_sem):
    cols = gt.shape[0]
    blk = 256
    starts = ([0] if cols % blk else []) + list(range(cols % blk, cols, blk))
    ends = starts[1:] + [cols]
    stores = []
    for i, (a, b) in enumerate(zip(starts, ends)):
        r = pl.ds(a, b - a)
        obuf[r, :] = jnp.dot(gt[r, :], x[...], preferred_element_type=F32)
        cp = pltpu.make_async_copy(obuf.at[r, :], o_hbm.at[r, :], o_sem.at[i])
        cp.start()
        stores.append(cp)
    for cp in stores:
        cp.wait()


def weight_grad(x_full, gt_blk):
    tokens, width = x_full.shape
    cols = gt_blk.shape[0]
    vmem = pl.BlockSpec(memory_space=pltpu.VMEM)
    return pl.pallas_call(
        weight_kernel,
        out_shape=jax.ShapeDtypeStruct((cols, width), F32),
        in_specs=[vmem] * 2,
        out_specs=pl.BlockSpec(memory_space=pltpu.HBM),
        scratch_shapes=[pltpu.VMEM((cols, width), F32), pltpu.SemaphoreType.DMA((16,))],
        compiler_params=pltpu.CompilerParams(vmem_limit_bytes=40 * 2**20),
        cost_estimate=pl.CostEstimate(flops=2 * tokens * width * cols, bytes_accessed=4 * width * cols,
                                      transcendentals=0),
        name="weight_grad",
    )(x_full, gt_blk)


def solution(mesh):
    n = mesh.shape["tp"]

    def per_device(x_blk, w_blk, grad_blk):
        x_full, gt_blk, own, plus, minus = exchange(x_blk, w_blk.T, grad_blk.T, n)
        from_left = lax.ppermute(plus, "tp", [(i, (i + 2) % n) for i in range(n)])
        from_right = lax.ppermute(minus, "tp", [(i, (i + n - 2) % n) for i in range(n)])
        grad_w = weight_grad(x_full, gt_blk).T
        grad_x = (own + from_left + from_right).astype(BF16)
        return grad_x, grad_w

    return jax.shard_map(
        per_device,
        mesh=mesh,
        in_specs=(P(("dp", "tp"), None), P(None, "tp"), P("dp", "tp")),
        out_specs=(P(("dp", "tp"), None), P("dp", "tp")),
        check_vma=False,
    )
```

```python
import functools

import jax
import jax.numpy as jnp
from jax import lax
from jax.experimental import pallas as pl
from jax.experimental.pallas import tpu as pltpu
from jax.sharding import PartitionSpec as P

MESH = pl.DeviceIdType.MESH
F32 = jnp.float32
BF16 = jnp.bfloat16


def exchange_kernel(n, groups, x_hbm, wt_hbm, gt_hbm, xf, gt, own, plus, minus,
                    wbuf, g, part, rbuf, opp_sum, u1buf,
                    x_sem, g_sem, w_sem, ag_send, ag_recv, pr_send, pr_recv,
                    d_send, d_recv, u_send, u_recv):
    rows, width = x_hbm.shape
    half = rows // 2
    nb = w_sem.shape[0]
    blk = width // nb
    me = lax.axis_index("tp")
    chips = n // 2
    chip, core = me // 2, lax.rem(me, 2)
    c_right, c_left = lax.rem(chip + 1, chips), lax.rem(chip + chips - 1, chips)
    c_opp = lax.rem(chip + 2, chips)
    right, left, opp = 2 * c_right + core, 2 * c_left + core, 2 * c_opp + core
    peer = 2 * chip + 1 - core
    lo, hi = pl.ds(0, half), pl.ds(half, half)

    def at(dev, part_of=0, size=rows):
        return xf.at[pl.ds(pl.multiple_of(dev * rows + part_of * half, half), size), :]

    def low(dev):
        return at(dev, 0, half)

    def high(dev):
        return at(dev, 1, half)

    own_x = pltpu.make_async_copy(x_hbm, at(me), x_sem)
    own_x.start()
    g_load = pltpu.make_async_copy(gt_hbm, gt, g_sem)
    g_load.start()
    ahead = 3

    def w_load(j):
        cols = pl.ds(j * blk, blk)
        return pltpu.make_async_copy(wt_hbm.at[:, cols], wbuf.at[:, cols], w_sem.at[j])

    for j in range(ahead):
        w_load(j).start()

    barrier = pltpu.get_barrier_semaphore()
    for dev in (left, right, peer):
        pl.semaphore_signal(barrier, inc=1, device_id={"tp": dev}, device_id_type=MESH)
    pl.semaphore_wait(barrier, 3)

    def send(src, dst, s_sem, r_sem, dev):
        cp = pltpu.make_async_remote_copy(src_ref=src, dst_ref=dst, send_sem=s_sem, recv_sem=r_sem,
                                          device_id={"tp": dev}, device_id_type=MESH)
        cp.start()
        return cp

    own_x.wait()
    ag = {}
    ag[0] = send(at(me), at(me), ag_send.at[0], ag_recv.at[0], right)
    ag[1] = send(at(me), at(me), ag_send.at[1], ag_recv.at[1], left)
    pr = {}
    pr[4] = send(at(me), at(me), pr_send.at[4], pr_recv.at[4], peer)

    def arrived(slot, block, onward=None):
        pltpu.make_async_remote_copy(src_ref=block, dst_ref=block, send_sem=ag_send.at[slot],
                                     recv_sem=ag_recv.at[slot], device_id={"tp": me}, device_id_type=MESH).wait_recv()
        if onward is not None:
            to, piece, dev = onward
            ag[to] = send(piece, piece, ag_send.at[to], ag_recv.at[to], dev)
        pr[slot] = send(block, block, pr_send.at[slot], pr_recv.at[slot], peer)

    g_load.wait()
    g[...] = gt[...].T

    d2d = {}

    def partial(j):
        w_load(j).wait()
        if j + ahead < nb:
            w_load(j + ahead).start()
        cols = pl.ds(j * blk, blk)
        t = jnp.dot(g[...], wbuf[:, cols], preferred_element_type=F32)
        t = t.reshape(chips, 2, rows, blk)
        for c in range(2):
            part[j, c] = t[:, c]
        d2d[j] = send(part.at[j, 1 - core], rbuf.at[j], d_send.at[j], d_recv.at[j], peer)

    u1 = []

    def chip_sum(js):
        for j in js:
            cols = pl.ds(j * blk, blk)
            d2d[j].wait_recv()
            opp_sum[j] = part[j, core, c_opp] + rbuf[j, c_opp]
            own[:, cols] = part[j, core, chip] + rbuf[j, chip]
            plus[:, cols] = part[j, core, c_right] + rbuf[j, c_right]
            minus[:, cols] = part[j, core, c_left] + rbuf[j, c_left]
        g0 = pl.ds(js[0], len(js))
        k = len(u1)
        u1.append((js, send(opp_sum.at[g0, lo], u1buf.at[g0, lo], u_send.at[0, k], u_recv.at[0, k], right),
                   send(opp_sum.at[g0, hi], u1buf.at[g0, hi], u_send.at[1, k], u_recv.at[1, k], left)))

    for j in range(5):
        partial(j)
    chip_sum(groups[0])
    partial(5)
    partial(6)
    arrived(0, at(left), (2, low(left), right))
    arrived(1, at(right), (3, high(right), left))
    chip_sum(groups[1])
    arrived(2, low(opp))
    arrived(3, high(opp))
    for js, from_left, from_right in u1:
        from_left.wait_recv()
        from_right.wait_recv()
        for j in js:
            cols = pl.ds(j * blk, blk)
            plus[lo, cols] += u1buf[j, lo]
            minus[hi, cols] += u1buf[j, hi]
    for cp in pr.values():
        cp.wait()
    for cp in ag.values():
        cp.wait_send()
    for cp in d2d.values():
        cp.wait_send()
    for _, a, b in u1:
        a.wait_send()
        b.wait_send()


def exchange(x_blk, wt_blk, gt_blk, n):
    rows, width = x_blk.shape
    cols, tokens = gt_blk.shape
    chips = n // 2
    nb = 7
    groups = ((0, 1, 2, 3), (4, 5, 6))
    hbm = pl.BlockSpec(memory_space=pltpu.HBM)
    vmem = pl.BlockSpec(memory_space=pltpu.VMEM)
    part = pltpu.VMEM((rows, width), F32)
    return pl.pallas_call(
        functools.partial(exchange_kernel, n, groups),
        out_shape=(pltpu.VMEM((tokens, width), BF16), pltpu.VMEM((cols, tokens), BF16), part, part, part),
        in_specs=[hbm] * 3,
        out_specs=(vmem,) * 5,
        scratch_shapes=[
            pltpu.VMEM((cols, width), BF16),
            pltpu.VMEM((tokens, cols), BF16),
            pltpu.VMEM((nb, 2, chips, rows, width // nb), F32),
            pltpu.VMEM((nb, chips, rows, width // nb), F32),
            pltpu.VMEM((nb, rows, width // nb), F32),
            pltpu.VMEM((nb, rows, width // nb), F32),
            pltpu.SemaphoreType.DMA,
            pltpu.SemaphoreType.DMA,
            pltpu.SemaphoreType.DMA((nb,)),
            pltpu.SemaphoreType.DMA((4,)),
            pltpu.SemaphoreType.DMA((4,)),
            pltpu.SemaphoreType.DMA((5,)),
            pltpu.SemaphoreType.DMA((5,)),
            pltpu.SemaphoreType.DMA((nb,)),
            pltpu.SemaphoreType.DMA((nb,)),
            pltpu.SemaphoreType.DMA((2, len(groups))),
            pltpu.SemaphoreType.DMA((2, len(groups))),
        ],
        compiler_params=pltpu.CompilerParams(collective_id=0, has_side_effects=True, vmem_limit_bytes=32 * 2**20),
        cost_estimate=pl.CostEstimate(flops=2 * tokens * width * cols, bytes_accessed=2 * width * cols,
                                      transcendentals=0),
        name="exchange",
    )(*(pltpu.with_memory_space_constraint(a, pltpu.HBM) for a in (x_blk, wt_blk, gt_blk)))


def weight_kernel(x, gt, o_hbm, obuf, o_sem):
    cols, width = o_hbm.shape
    blk = 256
    pieces = [(0, blk, c, min(512, width - c)) for c in range(0, width, 512)]
    pieces += [(r, min(blk, cols - r), 0, width) for r in range(blk, cols, blk)]
    stores = []
    for i, (r, nr, c, nc) in enumerate(pieces):
        rs, cs = pl.ds(r, nr), pl.ds(c, nc)
        obuf[rs, cs] = jnp.dot(gt[rs, :], x[:, cs], preferred_element_type=F32)
        cp = pltpu.make_async_copy(obuf.at[rs, cs], o_hbm.at[rs, cs], o_sem.at[i])
        cp.start()
        stores.append(cp)
    for cp in stores:
        cp.wait()


def weight_grad(x_full, gt_blk):
    tokens, width = x_full.shape
    cols = gt_blk.shape[0]
    vmem = pl.BlockSpec(memory_space=pltpu.VMEM)
    return pl.pallas_call(
        weight_kernel,
        out_shape=jax.ShapeDtypeStruct((cols, width), F32),
        in_specs=[vmem] * 2,
        out_specs=pl.BlockSpec(memory_space=pltpu.HBM),
        scratch_shapes=[pltpu.VMEM((cols, width), F32), pltpu.SemaphoreType.DMA((pl.cdiv(width, 512) + pl.cdiv(cols, 256),))],
        compiler_params=pltpu.CompilerParams(vmem_limit_bytes=40 * 2**20),
        cost_estimate=pl.CostEstimate(flops=2 * tokens * width * cols, bytes_accessed=4 * width * cols,
                                      transcendentals=0),
        name="weight_grad",
    )(x_full, gt_blk)


def solution(mesh):
    n = mesh.shape["tp"]

    def per_device(x_blk, w_blk, grad_blk):
        x_full, gt_blk, own, plus, minus = exchange(x_blk, w_blk.T, grad_blk.T, n)
        from_left = lax.ppermute(plus, "tp", [(i, (i + 2) % n) for i in range(n)])
        from_right = lax.ppermute(minus, "tp", [(i, (i + n - 2) % n) for i in range(n)])
        grad_w = weight_grad(x_full, gt_blk).T
        grad_x = (own + from_left + from_right).astype(BF16)
        return grad_x, grad_w

    return jax.shard_map(
        per_device,
        mesh=mesh,
        in_specs=(P(("dp", "tp"), None), P(None, "tp"), P("dp", "tp")),
        out_specs=(P(("dp", "tp"), None), P("dp", "tp")),
        check_vma=False,
    )
```

```python
import functools

import jax
import jax.numpy as jnp
from jax import lax
from jax.experimental import pallas as pl
from jax.experimental.pallas import tpu as pltpu
from jax.sharding import PartitionSpec as P

MESH = pl.DeviceIdType.MESH
F32 = jnp.float32
BF16 = jnp.bfloat16


def exchange_kernel(n, groups, x_hbm, wt_hbm, gt_hbm, xf, gt, own, first, second,
                    wbuf, g, part, rbuf, opp_sum, u1buf,
                    x_sem, g_sem, w_sem, ag_send, ag_recv, pr_send, pr_recv,
                    d_send, d_recv, u_send, u_recv):
    rows, width = x_hbm.shape
    half = rows // 2
    nb = w_sem.shape[0]
    blk = width // nb
    me = lax.axis_index("tp")
    chips = n // 2
    chip, core = me // 2, lax.rem(me, 2)
    c_right, c_left = lax.rem(chip + 1, chips), lax.rem(chip + chips - 1, chips)
    c_opp = lax.rem(chip + 2, chips)
    right, left, opp = 2 * c_right + core, 2 * c_left + core, 2 * c_opp + core
    peer = 2 * chip + 1 - core
    lo, hi = pl.ds(0, half), pl.ds(half, half)
    odd = lax.rem(chip, 2)
    c_first = odd * c_right + (1 - odd) * c_left
    c_second = odd * c_left + (1 - odd) * c_right
    r_first = pl.multiple_of((1 - odd) * half, half)
    r_second = pl.multiple_of(odd * half, half)

    def at(dev, part_of=0, size=rows):
        return xf.at[pl.ds(pl.multiple_of(dev * rows + part_of * half, half), size), :]

    def low(dev):
        return at(dev, 0, half)

    def high(dev):
        return at(dev, 1, half)

    own_x = pltpu.make_async_copy(x_hbm, at(me), x_sem)
    own_x.start()
    g_load = pltpu.make_async_copy(gt_hbm, gt, g_sem)
    g_load.start()
    ahead = 3

    def w_load(j):
        cols = pl.ds(j * blk, blk)
        return pltpu.make_async_copy(wt_hbm.at[:, cols], wbuf.at[:, cols], w_sem.at[j])

    for j in range(ahead):
        w_load(j).start()

    barrier = pltpu.get_barrier_semaphore()
    for dev in (left, right, peer):
        pl.semaphore_signal(barrier, inc=1, device_id={"tp": dev}, device_id_type=MESH)
    pl.semaphore_wait(barrier, 3)

    def send(src, dst, s_sem, r_sem, dev):
        cp = pltpu.make_async_remote_copy(src_ref=src, dst_ref=dst, send_sem=s_sem, recv_sem=r_sem,
                                          device_id={"tp": dev}, device_id_type=MESH)
        cp.start()
        return cp

    own_x.wait()
    ag = {}
    ag[0] = send(at(me), at(me), ag_send.at[0], ag_recv.at[0], right)
    ag[1] = send(at(me), at(me), ag_send.at[1], ag_recv.at[1], left)
    pr = {}
    pr[4] = send(at(me), at(me), pr_send.at[4], pr_recv.at[4], peer)

    def arrived(slot, block, onward=None):
        pltpu.make_async_remote_copy(src_ref=block, dst_ref=block, send_sem=ag_send.at[slot],
                                     recv_sem=ag_recv.at[slot], device_id={"tp": me}, device_id_type=MESH).wait_recv()
        if onward is not None:
            to, piece, dev = onward
            ag[to] = send(piece, piece, ag_send.at[to], ag_recv.at[to], dev)
        pr[slot] = send(block, block, pr_send.at[slot], pr_recv.at[slot], peer)

    g_load.wait()
    g[...] = gt[...].T

    d2d = {}

    def partial(j):
        w_load(j).wait()
        if j + ahead < nb:
            w_load(j + ahead).start()
        cols = pl.ds(j * blk, blk)
        t = jnp.dot(g[...], wbuf[:, cols], preferred_element_type=F32)
        t = t.reshape(chips, 2, rows, blk)
        for c in range(2):
            part[j, c] = t[:, c]
        d2d[j] = send(part.at[j, 1 - core], rbuf.at[j], d_send.at[j], d_recv.at[j], peer)

    u1 = []

    def chip_sum(js):
        for j in js:
            cols = pl.ds(j * blk, blk)
            d2d[j].wait_recv()
            opp_sum[j] = part[j, core, c_opp] + rbuf[j, c_opp]
            own[:, cols] = part[j, core, chip] + rbuf[j, chip]
            first[:, cols] = part[j, core, c_first] + rbuf[j, c_first]
            second[:, cols] = part[j, core, c_second] + rbuf[j, c_second]
        g0 = pl.ds(js[0], len(js))
        k = len(u1)
        u1.append((js, send(opp_sum.at[g0, lo], u1buf.at[g0, lo], u_send.at[0, k], u_recv.at[0, k], right),
                   send(opp_sum.at[g0, hi], u1buf.at[g0, hi], u_send.at[1, k], u_recv.at[1, k], left)))

    for j in range(5):
        partial(j)
    chip_sum(groups[0])
    partial(5)
    partial(6)
    arrived(0, at(left), (2, low(left), right))
    arrived(1, at(right), (3, high(right), left))
    chip_sum(groups[1])
    arrived(2, low(opp))
    arrived(3, high(opp))
    for js, from_left, from_right in u1:
        from_left.wait_recv()
        from_right.wait_recv()
        for j in js:
            cols = pl.ds(j * blk, blk)
            first[pl.ds(r_first, half), cols] += u1buf[j, pl.ds(r_first, half)]
            second[pl.ds(r_second, half), cols] += u1buf[j, pl.ds(r_second, half)]
    for cp in pr.values():
        cp.wait()
    for cp in ag.values():
        cp.wait_send()
    for cp in d2d.values():
        cp.wait_send()
    for _, a, b in u1:
        a.wait_send()
        b.wait_send()


def exchange(x_blk, wt_blk, gt_blk, n):
    rows, width = x_blk.shape
    cols, tokens = gt_blk.shape
    chips = n // 2
    nb = 7
    groups = ((0, 1, 2, 3), (4, 5, 6))
    hbm = pl.BlockSpec(memory_space=pltpu.HBM)
    vmem = pl.BlockSpec(memory_space=pltpu.VMEM)
    part = pltpu.VMEM((rows, width), F32)
    return pl.pallas_call(
        functools.partial(exchange_kernel, n, groups),
        out_shape=(pltpu.VMEM((tokens, width), BF16), pltpu.VMEM((cols, tokens), BF16), part, part, part),
        in_specs=[hbm] * 3,
        out_specs=(vmem,) * 5,
        scratch_shapes=[
            pltpu.VMEM((cols, width), BF16),
            pltpu.VMEM((tokens, cols), BF16),
            pltpu.VMEM((nb, 2, chips, rows, width // nb), F32),
            pltpu.VMEM((nb, chips, rows, width // nb), F32),
            pltpu.VMEM((nb, rows, width // nb), F32),
            pltpu.VMEM((nb, rows, width // nb), F32),
            pltpu.SemaphoreType.DMA,
            pltpu.SemaphoreType.DMA,
            pltpu.SemaphoreType.DMA((nb,)),
            pltpu.SemaphoreType.DMA((4,)),
            pltpu.SemaphoreType.DMA((4,)),
            pltpu.SemaphoreType.DMA((5,)),
            pltpu.SemaphoreType.DMA((5,)),
            pltpu.SemaphoreType.DMA((nb,)),
            pltpu.SemaphoreType.DMA((nb,)),
            pltpu.SemaphoreType.DMA((2, len(groups))),
            pltpu.SemaphoreType.DMA((2, len(groups))),
        ],
        compiler_params=pltpu.CompilerParams(collective_id=0, has_side_effects=True, vmem_limit_bytes=32 * 2**20),
        cost_estimate=pl.CostEstimate(flops=2 * tokens * width * cols, bytes_accessed=2 * width * cols,
                                      transcendentals=0),
        name="exchange",
    )(*(pltpu.with_memory_space_constraint(a, pltpu.HBM) for a in (x_blk, wt_blk, gt_blk)))


def weight_kernel(x, gt, o_hbm, obuf, o_sem):
    cols, width = o_hbm.shape
    blk = 256
    pieces = [(0, blk, c, min(512, width - c)) for c in range(0, width, 512)]
    pieces += [(r, min(blk, cols - r), 0, width) for r in range(blk, cols, blk)]
    stores = []
    for i, (r, nr, c, nc) in enumerate(pieces):
        rs, cs = pl.ds(r, nr), pl.ds(c, nc)
        obuf[rs, cs] = jnp.dot(gt[rs, :], x[:, cs], preferred_element_type=F32)
        cp = pltpu.make_async_copy(obuf.at[rs, cs], o_hbm.at[rs, cs], o_sem.at[i])
        cp.start()
        stores.append(cp)
    for cp in stores:
        cp.wait()


def weight_grad(x_full, gt_blk):
    tokens, width = x_full.shape
    cols = gt_blk.shape[0]
    vmem = pl.BlockSpec(memory_space=pltpu.VMEM)
    return pl.pallas_call(
        weight_kernel,
        out_shape=jax.ShapeDtypeStruct((cols, width), F32),
        in_specs=[vmem] * 2,
        out_specs=pl.BlockSpec(memory_space=pltpu.HBM),
        scratch_shapes=[pltpu.VMEM((cols, width), F32), pltpu.SemaphoreType.DMA((pl.cdiv(width, 512) + pl.cdiv(cols, 256),))],
        compiler_params=pltpu.CompilerParams(vmem_limit_bytes=40 * 2**20),
        cost_estimate=pl.CostEstimate(flops=2 * tokens * width * cols, bytes_accessed=4 * width * cols,
                                      transcendentals=0),
        name="weight_grad",
    )(x_full, gt_blk)


def solution(mesh):
    n = mesh.shape["tp"]

    def per_device(x_blk, w_blk, grad_blk):
        x_full, gt_blk, own, first, second = exchange(x_blk, w_blk.T, grad_blk.T, n)

        def swap(part, start):
            pairs = []
            for c in range(start, start + n // 2, 2):
                for core in range(2):
                    a, b = (2 * c + core) % n, (2 * c + 2 + core) % n
                    pairs += [(a, b), (b, a)]
            return lax.ppermute(part, "tp", pairs)

        got_first = swap(first, 1)
        got_second = swap(second, 0)
        grad_w = weight_grad(x_full, gt_blk).T
        grad_x = (own + got_first + got_second).astype(BF16)
        return grad_x, grad_w

    return jax.shard_map(
        per_device,
        mesh=mesh,
        in_specs=(P(("dp", "tp"), None), P(None, "tp"), P("dp", "tp")),
        out_specs=(P(("dp", "tp"), None), P("dp", "tp")),
        check_vma=False,
    )
```

```python
import functools

import jax
import jax.numpy as jnp
from jax import lax
from jax.experimental import pallas as pl
from jax.experimental.pallas import tpu as pltpu
from jax.sharding import PartitionSpec as P

MESH = pl.DeviceIdType.MESH
F32 = jnp.float32
BF16 = jnp.bfloat16


def exchange_kernel(n, groups, x_hbm, wt_hbm, gt_hbm, xf, gt, own, first, second,
                    wbuf, g, part, rbuf, opp_sum, u1buf,
                    x_sem, g_sem, w_sem, ag_send, ag_recv, pr_send, pr_recv,
                    d_send, d_recv, u_send, u_recv):
    rows, width = x_hbm.shape
    half = rows // 2
    nb = w_sem.shape[0]
    blk = width // nb
    me = lax.axis_index("tp")
    chips = n // 2
    chip, core = me // 2, lax.rem(me, 2)
    c_right, c_left = lax.rem(chip + 1, chips), lax.rem(chip + chips - 1, chips)
    c_opp = lax.rem(chip + 2, chips)
    right, left, opp = 2 * c_right + core, 2 * c_left + core, 2 * c_opp + core
    peer = 2 * chip + 1 - core
    lo, hi = pl.ds(0, half), pl.ds(half, half)
    odd = lax.rem(chip, 2)
    c_first = odd * c_right + (1 - odd) * c_left
    c_second = odd * c_left + (1 - odd) * c_right
    r_first = pl.multiple_of((1 - odd) * half, half)
    r_second = pl.multiple_of(odd * half, half)

    def at(dev, part_of=0, size=rows):
        return xf.at[pl.ds(pl.multiple_of(dev * rows + part_of * half, half), size), :]

    def low(dev):
        return at(dev, 0, half)

    def high(dev):
        return at(dev, 1, half)

    own_x = pltpu.make_async_copy(x_hbm, at(me), x_sem)
    own_x.start()
    g_load = pltpu.make_async_copy(gt_hbm, gt, g_sem)
    g_load.start()
    ahead = 3

    def w_load(j):
        cols = pl.ds(j * blk, blk)
        return pltpu.make_async_copy(wt_hbm.at[:, cols], wbuf.at[:, cols], w_sem.at[j])

    for j in range(ahead):
        w_load(j).start()

    barrier = pltpu.get_barrier_semaphore()
    for dev in (left, right, peer):
        pl.semaphore_signal(barrier, inc=1, device_id={"tp": dev}, device_id_type=MESH)
    pl.semaphore_wait(barrier, 3)

    def send(src, dst, s_sem, r_sem, dev):
        cp = pltpu.make_async_remote_copy(src_ref=src, dst_ref=dst, send_sem=s_sem, recv_sem=r_sem,
                                          device_id={"tp": dev}, device_id_type=MESH)
        cp.start()
        return cp

    own_x.wait()
    ag = {}
    ag[0] = send(at(me), at(me), ag_send.at[0], ag_recv.at[0], right)
    ag[1] = send(at(me), at(me), ag_send.at[1], ag_recv.at[1], left)
    pr = {}
    pr[4] = send(at(me), at(me), pr_send.at[4], pr_recv.at[4], peer)

    def arrived(slot, block, onward=None):
        pltpu.make_async_remote_copy(src_ref=block, dst_ref=block, send_sem=ag_send.at[slot],
                                     recv_sem=ag_recv.at[slot], device_id={"tp": me}, device_id_type=MESH).wait_recv()
        if onward is not None:
            to, piece, dev = onward
            ag[to] = send(piece, piece, ag_send.at[to], ag_recv.at[to], dev)
        pr[slot] = send(block, block, pr_send.at[slot], pr_recv.at[slot], peer)

    g_load.wait()
    g[...] = gt[...].T

    d2d = {}

    def partial(j):
        w_load(j).wait()
        if j + ahead < nb:
            w_load(j + ahead).start()
        cols = pl.ds(j * blk, blk)
        t = jnp.dot(g[...], wbuf[:, cols], preferred_element_type=F32)
        t = t.reshape(chips, 2, rows, blk)
        for c in range(2):
            part[j, c] = t[:, c]
        d2d[j] = send(part.at[j, 1 - core], rbuf.at[j], d_send.at[j], d_recv.at[j], peer)

    u1 = []

    def chip_sum(js):
        for j in js:
            cols = pl.ds(j * blk, blk)
            d2d[j].wait_recv()
            opp_sum[j] = part[j, core, c_opp] + rbuf[j, c_opp]
            own[:, cols] = part[j, core, chip] + rbuf[j, chip]
            first[:, cols] = part[j, core, c_first] + rbuf[j, c_first]
            second[:, cols] = part[j, core, c_second] + rbuf[j, c_second]
        g0 = pl.ds(js[0], len(js))
        k = len(u1)
        u1.append((js, send(opp_sum.at[g0, lo], u1buf.at[g0, lo], u_send.at[0, k], u_recv.at[0, k], right),
                   send(opp_sum.at[g0, hi], u1buf.at[g0, hi], u_send.at[1, k], u_recv.at[1, k], left)))

    partial(0)
    partial(1)
    partial(2)
    chip_sum(groups[0])
    partial(3)
    partial(4)
    chip_sum(groups[1])
    partial(5)
    partial(6)
    arrived(0, at(left), (2, low(left), right))
    arrived(1, at(right), (3, high(right), left))
    chip_sum(groups[2])
    arrived(2, low(opp))
    arrived(3, high(opp))
    for js, from_left, from_right in u1:
        from_left.wait_recv()
        from_right.wait_recv()
        for j in js:
            cols = pl.ds(j * blk, blk)
            first[pl.ds(r_first, half), cols] += u1buf[j, pl.ds(r_first, half)]
            second[pl.ds(r_second, half), cols] += u1buf[j, pl.ds(r_second, half)]
    for cp in pr.values():
        cp.wait()
    for cp in ag.values():
        cp.wait_send()
    for cp in d2d.values():
        cp.wait_send()
    for _, a, b in u1:
        a.wait_send()
        b.wait_send()


def exchange(x_blk, wt_blk, gt_blk, n):
    rows, width = x_blk.shape
    cols, tokens = gt_blk.shape
    chips = n // 2
    nb = 7
    groups = ((0, 1), (2, 3), (4, 5, 6))
    hbm = pl.BlockSpec(memory_space=pltpu.HBM)
    vmem = pl.BlockSpec(memory_space=pltpu.VMEM)
    part = pltpu.VMEM((rows, width), F32)
    return pl.pallas_call(
        functools.partial(exchange_kernel, n, groups),
        out_shape=(pltpu.VMEM((tokens, width), BF16), pltpu.VMEM((cols, tokens), BF16), part, part, part),
        in_specs=[hbm] * 3,
        out_specs=(vmem,) * 5,
        scratch_shapes=[
            pltpu.VMEM((cols, width), BF16),
            pltpu.VMEM((tokens, cols), BF16),
            pltpu.VMEM((nb, 2, chips, rows, width // nb), F32),
            pltpu.VMEM((nb, chips, rows, width // nb), F32),
            pltpu.VMEM((nb, rows, width // nb), F32),
            pltpu.VMEM((nb, rows, width // nb), F32),
            pltpu.SemaphoreType.DMA,
            pltpu.SemaphoreType.DMA,
            pltpu.SemaphoreType.DMA((nb,)),
            pltpu.SemaphoreType.DMA((4,)),
            pltpu.SemaphoreType.DMA((4,)),
            pltpu.SemaphoreType.DMA((5,)),
            pltpu.SemaphoreType.DMA((5,)),
            pltpu.SemaphoreType.DMA((nb,)),
            pltpu.SemaphoreType.DMA((nb,)),
            pltpu.SemaphoreType.DMA((2, len(groups))),
            pltpu.SemaphoreType.DMA((2, len(groups))),
        ],
        compiler_params=pltpu.CompilerParams(collective_id=0, has_side_effects=True, vmem_limit_bytes=32 * 2**20),
        cost_estimate=pl.CostEstimate(flops=2 * tokens * width * cols, bytes_accessed=2 * width * cols,
                                      transcendentals=0),
        name="exchange",
    )(*(pltpu.with_memory_space_constraint(a, pltpu.HBM) for a in (x_blk, wt_blk, gt_blk)))


def weight_kernel(x, gt, o_hbm, obuf, o_sem):
    cols, width = o_hbm.shape
    blk = 256
    pieces = [(0, blk, c, min(512, width - c)) for c in range(0, width, 512)]
    pieces += [(r, min(blk, cols - r), 0, width) for r in range(blk, cols, blk)]
    stores = []
    for i, (r, nr, c, nc) in enumerate(pieces):
        rs, cs = pl.ds(r, nr), pl.ds(c, nc)
        obuf[rs, cs] = jnp.dot(gt[rs, :], x[:, cs], preferred_element_type=F32)
        cp = pltpu.make_async_copy(obuf.at[rs, cs], o_hbm.at[rs, cs], o_sem.at[i])
        cp.start()
        stores.append(cp)
    for cp in stores:
        cp.wait()


def weight_grad(x_full, gt_blk):
    tokens, width = x_full.shape
    cols = gt_blk.shape[0]
    vmem = pl.BlockSpec(memory_space=pltpu.VMEM)
    return pl.pallas_call(
        weight_kernel,
        out_shape=jax.ShapeDtypeStruct((cols, width), F32),
        in_specs=[vmem] * 2,
        out_specs=pl.BlockSpec(memory_space=pltpu.HBM),
        scratch_shapes=[pltpu.VMEM((cols, width), F32), pltpu.SemaphoreType.DMA((pl.cdiv(width, 512) + pl.cdiv(cols, 256),))],
        compiler_params=pltpu.CompilerParams(vmem_limit_bytes=40 * 2**20),
        cost_estimate=pl.CostEstimate(flops=2 * tokens * width * cols, bytes_accessed=4 * width * cols,
                                      transcendentals=0),
        name="weight_grad",
    )(x_full, gt_blk)


def solution(mesh):
    n = mesh.shape["tp"]

    def per_device(x_blk, w_blk, grad_blk):
        x_full, gt_blk, own, first, second = exchange(x_blk, w_blk.T, grad_blk.T, n)

        def swap(part, start):
            pairs = []
            for c in range(start, start + n // 2, 2):
                for core in range(2):
                    a, b = (2 * c + core) % n, (2 * c + 2 + core) % n
                    pairs += [(a, b), (b, a)]
            return lax.ppermute(part, "tp", pairs)

        got_first = swap(first, 1)
        got_second = swap(second, 0)
        grad_w = weight_grad(x_full, gt_blk).T
        grad_x = (own + got_first + got_second).astype(BF16)
        return grad_x, grad_w

    return jax.shard_map(
        per_device,
        mesh=mesh,
        in_specs=(P(("dp", "tp"), None), P(None, "tp"), P("dp", "tp")),
        out_specs=(P(("dp", "tp"), None), P("dp", "tp")),
        check_vma=False,
    )
```

```python
import functools

import jax
import jax.numpy as jnp
from jax import lax
from jax.experimental import pallas as pl
from jax.experimental.pallas import tpu as pltpu
from jax.sharding import PartitionSpec as P

MESH = pl.DeviceIdType.MESH
F32 = jnp.float32
BF16 = jnp.bfloat16


def exchange_kernel(n, groups, x_hbm, wt_hbm, gt_hbm, xf, gt, own, first, second,
                    wbuf, g, part, rbuf, opp_sum, u1buf,
                    x_sem, g_sem, w_sem, ag_send, ag_recv, pr_send, pr_recv,
                    d_send, d_recv, u_send, u_recv):
    rows, width = x_hbm.shape
    half = rows // 2
    nb = w_sem.shape[0]
    blk = width // nb
    me = lax.axis_index("tp")
    chips = n // 2
    chip, core = me // 2, lax.rem(me, 2)
    c_right, c_left = lax.rem(chip + 1, chips), lax.rem(chip + chips - 1, chips)
    c_opp = lax.rem(chip + 2, chips)
    right, left, opp = 2 * c_right + core, 2 * c_left + core, 2 * c_opp + core
    peer = 2 * chip + 1 - core
    lo, hi = pl.ds(0, half), pl.ds(half, half)
    odd = lax.rem(chip, 2)
    c_first = odd * c_right + (1 - odd) * c_left
    c_second = odd * c_left + (1 - odd) * c_right
    r_first = pl.multiple_of((1 - odd) * half, half)
    r_second = pl.multiple_of(odd * half, half)

    def at(dev, part_of=0, size=rows):
        return xf.at[pl.ds(pl.multiple_of(dev * rows + part_of * half, half), size), :]

    def low(dev):
        return at(dev, 0, half)

    def high(dev):
        return at(dev, 1, half)

    barrier = pltpu.get_barrier_semaphore()
    for dev in (left, right, peer):
        pl.semaphore_signal(barrier, inc=1, device_id={"tp": dev}, device_id_type=MESH)

    own_x = pltpu.make_async_copy(x_hbm, at(me), x_sem)
    own_x.start()
    g_load = pltpu.make_async_copy(gt_hbm, gt, g_sem)
    g_load.start()
    ahead = 5

    def w_load(j):
        cols = pl.ds(j * blk, blk)
        return pltpu.make_async_copy(wt_hbm.at[:, cols], wbuf.at[:, cols], w_sem.at[j])

    for j in range(ahead):
        w_load(j).start()

    pl.semaphore_wait(barrier, 3)

    def send(src, dst, s_sem, r_sem, dev):
        cp = pltpu.make_async_remote_copy(src_ref=src, dst_ref=dst, send_sem=s_sem, recv_sem=r_sem,
                                          device_id={"tp": dev}, device_id_type=MESH)
        cp.start()
        return cp

    own_x.wait()
    ag = {}
    ag[0] = send(at(me), at(me), ag_send.at[0], ag_recv.at[0], right)
    ag[1] = send(at(me), at(me), ag_send.at[1], ag_recv.at[1], left)
    pr = {}
    pr[4] = send(at(me), at(me), pr_send.at[4], pr_recv.at[4], peer)

    def arrived(slot, block, onward=None):
        pltpu.make_async_remote_copy(src_ref=block, dst_ref=block, send_sem=ag_send.at[slot],
                                     recv_sem=ag_recv.at[slot], device_id={"tp": me}, device_id_type=MESH).wait_recv()
        if onward is not None:
            to, piece, dev = onward
            ag[to] = send(piece, piece, ag_send.at[to], ag_recv.at[to], dev)
        pr[slot] = send(block, block, pr_send.at[slot], pr_recv.at[slot], peer)

    g_load.wait()
    g[...] = gt[...].T

    d2d = {}

    def partial(j):
        w_load(j).wait()
        if j + ahead < nb:
            w_load(j + ahead).start()
        cols = pl.ds(j * blk, blk)
        t = jnp.dot(g[...], wbuf[:, cols], preferred_element_type=F32)
        t = t.reshape(chips, 2, rows, blk)
        for c in range(2):
            part[j, c] = t[:, c]
        d2d[j] = send(part.at[j, 1 - core], rbuf.at[j], d_send.at[j], d_recv.at[j], peer)

    u1 = []

    def chip_sum(js):
        for j in js:
            cols = pl.ds(j * blk, blk)
            d2d[j].wait_recv()
            opp_sum[j] = part[j, core, c_opp] + rbuf[j, c_opp]
            own[:, cols] = part[j, core, chip] + rbuf[j, chip]
            first[:, cols] = part[j, core, c_first] + rbuf[j, c_first]
            second[:, cols] = part[j, core, c_second] + rbuf[j, c_second]
        g0 = pl.ds(js[0], len(js))
        k = len(u1)
        u1.append((js, send(opp_sum.at[g0, lo], u1buf.at[g0, lo], u_send.at[0, k], u_recv.at[0, k], right),
                   send(opp_sum.at[g0, hi], u1buf.at[g0, hi], u_send.at[1, k], u_recv.at[1, k], left)))

    partial(0)
    partial(1)
    partial(2)
    chip_sum(groups[0])
    partial(3)
    partial(4)
    chip_sum(groups[1])
    partial(5)
    partial(6)
    arrived(0, at(left), (2, low(left), right))
    arrived(1, at(right), (3, high(right), left))
    chip_sum(groups[2])
    arrived(2, low(opp))
    arrived(3, high(opp))
    for cp in pr.values():
        cp.wait()
    for cp in ag.values():
        cp.wait_send()
    for cp in d2d.values():
        cp.wait_send()
    for _, a, b in u1:
        a.wait_send()
        b.wait_send()
    for js, from_left, from_right in u1:
        from_left.wait_recv()
        from_right.wait_recv()
        for j in js:
            cols = pl.ds(j * blk, blk)
            first[pl.ds(r_first, half), cols] += u1buf[j, pl.ds(r_first, half)]
            second[pl.ds(r_second, half), cols] += u1buf[j, pl.ds(r_second, half)]


def exchange(x_blk, wt_blk, gt_blk, n):
    rows, width = x_blk.shape
    cols, tokens = gt_blk.shape
    chips = n // 2
    nb = 7
    groups = ((0, 1), (2, 3), (4, 5, 6))
    hbm = pl.BlockSpec(memory_space=pltpu.HBM)
    vmem = pl.BlockSpec(memory_space=pltpu.VMEM)
    part = pltpu.VMEM((rows, width), F32)
    return pl.pallas_call(
        functools.partial(exchange_kernel, n, groups),
        out_shape=(pltpu.VMEM((tokens, width), BF16), pltpu.VMEM((cols, tokens), BF16), part, part, part),
        in_specs=[hbm] * 3,
        out_specs=(vmem,) * 5,
        scratch_shapes=[
            pltpu.VMEM((cols, width), BF16),
            pltpu.VMEM((tokens, cols), BF16),
            pltpu.VMEM((nb, 2, chips, rows, width // nb), F32),
            pltpu.VMEM((nb, chips, rows, width // nb), F32),
            pltpu.VMEM((nb, rows, width // nb), F32),
            pltpu.VMEM((nb, rows, width // nb), F32),
            pltpu.SemaphoreType.DMA,
            pltpu.SemaphoreType.DMA,
            pltpu.SemaphoreType.DMA((nb,)),
            pltpu.SemaphoreType.DMA((4,)),
            pltpu.SemaphoreType.DMA((4,)),
            pltpu.SemaphoreType.DMA((5,)),
            pltpu.SemaphoreType.DMA((5,)),
            pltpu.SemaphoreType.DMA((nb,)),
            pltpu.SemaphoreType.DMA((nb,)),
            pltpu.SemaphoreType.DMA((2, len(groups))),
            pltpu.SemaphoreType.DMA((2, len(groups))),
        ],
        compiler_params=pltpu.CompilerParams(collective_id=0, has_side_effects=True, vmem_limit_bytes=32 * 2**20),
        cost_estimate=pl.CostEstimate(flops=2 * tokens * width * cols, bytes_accessed=2 * width * cols,
                                      transcendentals=0),
        name="exchange",
    )(*(pltpu.with_memory_space_constraint(a, pltpu.HBM) for a in (x_blk, wt_blk, gt_blk)))


def weight_kernel(x, gt, o_hbm, obuf, o_sem):
    cols, width = o_hbm.shape
    blk = 256
    pieces = [(0, blk, c, min(512, width - c)) for c in range(0, width, 512)]
    pieces += [(r, min(blk, cols - r), 0, width) for r in range(blk, cols, blk)]
    stores = []
    for i, (r, nr, c, nc) in enumerate(pieces):
        rs, cs = pl.ds(r, nr), pl.ds(c, nc)
        obuf[rs, cs] = jnp.dot(gt[rs, :], x[:, cs], preferred_element_type=F32)
        cp = pltpu.make_async_copy(obuf.at[rs, cs], o_hbm.at[rs, cs], o_sem.at[i])
        cp.start()
        stores.append(cp)
    for cp in stores:
        cp.wait()


def weight_grad(x_full, gt_blk):
    tokens, width = x_full.shape
    cols = gt_blk.shape[0]
    vmem = pl.BlockSpec(memory_space=pltpu.VMEM)
    return pl.pallas_call(
        weight_kernel,
        out_shape=jax.ShapeDtypeStruct((cols, width), F32),
        in_specs=[vmem] * 2,
        out_specs=pl.BlockSpec(memory_space=pltpu.HBM),
        scratch_shapes=[pltpu.VMEM((cols, width), F32), pltpu.SemaphoreType.DMA((pl.cdiv(width, 512) + pl.cdiv(cols, 256),))],
        compiler_params=pltpu.CompilerParams(vmem_limit_bytes=40 * 2**20),
        cost_estimate=pl.CostEstimate(flops=2 * tokens * width * cols, bytes_accessed=4 * width * cols,
                                      transcendentals=0),
        name="weight_grad",
    )(x_full, gt_blk)


def solution(mesh):
    n = mesh.shape["tp"]

    def per_device(x_blk, w_blk, grad_blk):
        x_full, gt_blk, own, first, second = exchange(x_blk, w_blk.T, grad_blk.T, n)

        def swap(part, start):
            pairs = []
            for c in range(start, start + n // 2, 2):
                for core in range(2):
                    a, b = (2 * c + core) % n, (2 * c + 2 + core) % n
                    pairs += [(a, b), (b, a)]
            return lax.ppermute(part, "tp", pairs)

        got_first = swap(first, 1)
        got_second = swap(second, 0)
        grad_w = weight_grad(x_full, gt_blk).T
        grad_x = (own + got_first + got_second).astype(BF16)
        return grad_x, grad_w

    return jax.shard_map(
        per_device,
        mesh=mesh,
        in_specs=(P(("dp", "tp"), None), P(None, "tp"), P("dp", "tp")),
        out_specs=(P(("dp", "tp"), None), P("dp", "tp")),
        check_vma=False,
    )
```

```python
import functools

import jax
import jax.numpy as jnp
from jax import lax
from jax.experimental import pallas as pl
from jax.experimental.pallas import tpu as pltpu
from jax.sharding import PartitionSpec as P

MESH = pl.DeviceIdType.MESH
F32 = jnp.float32
BF16 = jnp.bfloat16


def exchange_kernel(n, groups, x_hbm, wt_hbm, gt_hbm, xf, gt, own, first, second,
                    wbuf, g, part, rbuf, opp_sum, u1buf,
                    x_sem, g_sem, w_sem, ag_send, ag_recv, pr_send, pr_recv,
                    d_send, d_recv, u_send, u_recv):
    rows, width = x_hbm.shape
    half = rows // 2
    nb = w_sem.shape[0]
    blk = width // nb
    me = lax.axis_index("tp")
    chips = n // 2
    chip, core = me // 2, lax.rem(me, 2)
    c_right, c_left = lax.rem(chip + 1, chips), lax.rem(chip + chips - 1, chips)
    c_opp = lax.rem(chip + 2, chips)
    right, left, opp = 2 * c_right + core, 2 * c_left + core, 2 * c_opp + core
    peer = 2 * chip + 1 - core
    lo, hi = pl.ds(0, half), pl.ds(half, half)
    odd = lax.rem(chip, 2)
    c_first = odd * c_right + (1 - odd) * c_left
    c_second = odd * c_left + (1 - odd) * c_right
    r_first = pl.multiple_of((1 - odd) * half, half)
    r_second = pl.multiple_of(odd * half, half)

    def at(dev, part_of=0, size=rows):
        return xf.at[pl.ds(pl.multiple_of(dev * rows + part_of * half, half), size), :]

    def low(dev):
        return at(dev, 0, half)

    def high(dev):
        return at(dev, 1, half)

    barrier = pltpu.get_barrier_semaphore()
    for dev in (left, right, peer):
        pl.semaphore_signal(barrier, inc=1, device_id={"tp": dev}, device_id_type=MESH)

    own_x = pltpu.make_async_copy(x_hbm, at(me), x_sem)
    own_x.start()
    g_load = pltpu.make_async_copy(gt_hbm, gt, g_sem)
    g_load.start()
    ahead = 2

    def w_load(j):
        cols = pl.ds(j * blk, blk)
        return pltpu.make_async_copy(wt_hbm.at[:, cols], wbuf.at[:, cols], w_sem.at[j])

    for j in range(ahead):
        w_load(j).start()

    pl.semaphore_wait(barrier, 3)

    def send(src, dst, s_sem, r_sem, dev):
        cp = pltpu.make_async_remote_copy(src_ref=src, dst_ref=dst, send_sem=s_sem, recv_sem=r_sem,
                                          device_id={"tp": dev}, device_id_type=MESH)
        cp.start()
        return cp

    own_x.wait()
    ag = {}
    ag[0] = send(at(me), at(me), ag_send.at[0], ag_recv.at[0], right)
    ag[1] = send(at(me), at(me), ag_send.at[1], ag_recv.at[1], left)
    pr = {}
    pr[4] = send(at(me), at(me), pr_send.at[4], pr_recv.at[4], peer)

    def arrived(slot, block, onward=None):
        pltpu.make_async_remote_copy(src_ref=block, dst_ref=block, send_sem=ag_send.at[slot],
                                     recv_sem=ag_recv.at[slot], device_id={"tp": me}, device_id_type=MESH).wait_recv()
        if onward is not None:
            to, piece, dev = onward
            ag[to] = send(piece, piece, ag_send.at[to], ag_recv.at[to], dev)
        pr[slot] = send(block, block, pr_send.at[slot], pr_recv.at[slot], peer)

    g_load.wait()
    g[...] = gt[...].T

    d2d = {}

    def partial(j):
        w_load(j).wait()
        if j + ahead < nb:
            w_load(j + ahead).start()
        cols = pl.ds(j * blk, blk)
        t = jnp.dot(g[...], wbuf[:, cols], preferred_element_type=F32)
        t = t.reshape(chips, 2, rows, blk)
        for c in range(2):
            part[j, c] = t[:, c]
        d2d[j] = send(part.at[j, 1 - core], rbuf.at[j], d_send.at[j], d_recv.at[j], peer)

    u1 = []

    def chip_sum(js):
        for j in js:
            cols = pl.ds(j * blk, blk)
            d2d[j].wait_recv()
            opp_sum[j] = part[j, core, c_opp] + rbuf[j, c_opp]
            own[:, cols] = part[j, core, chip] + rbuf[j, chip]
            first[:, cols] = part[j, core, c_first] + rbuf[j, c_first]
            second[:, cols] = part[j, core, c_second] + rbuf[j, c_second]
        g0 = pl.ds(js[0], len(js))
        k = len(u1)
        u1.append((js, send(opp_sum.at[g0, lo], u1buf.at[g0, lo], u_send.at[0, k], u_recv.at[0, k], right),
                   send(opp_sum.at[g0, hi], u1buf.at[g0, hi], u_send.at[1, k], u_recv.at[1, k], left)))

    partial(0)
    partial(1)
    partial(2)
    chip_sum(groups[0])
    partial(3)
    partial(4)
    chip_sum(groups[1])
    partial(5)
    partial(6)
    arrived(0, at(left), (2, low(left), right))
    arrived(1, at(right), (3, high(right), left))
    chip_sum(groups[2])
    arrived(2, low(opp))
    arrived(3, high(opp))
    for cp in pr.values():
        cp.wait()
    for cp in ag.values():
        cp.wait_send()
    for cp in d2d.values():
        cp.wait_send()
    for _, a, b in u1:
        a.wait_send()
        b.wait_send()
    for js, from_left, from_right in u1:
        from_left.wait_recv()
        from_right.wait_recv()
        for j in js:
            cols = pl.ds(j * blk, blk)
            first[pl.ds(r_first, half), cols] += u1buf[j, pl.ds(r_first, half)]
            second[pl.ds(r_second, half), cols] += u1buf[j, pl.ds(r_second, half)]


def exchange(x_blk, wt_blk, gt_blk, n):
    rows, width = x_blk.shape
    cols, tokens = gt_blk.shape
    chips = n // 2
    nb = 7
    groups = ((0, 1), (2, 3), (4, 5, 6))
    hbm = pl.BlockSpec(memory_space=pltpu.HBM)
    vmem = pl.BlockSpec(memory_space=pltpu.VMEM)
    part = pltpu.VMEM((rows, width), F32)
    return pl.pallas_call(
        functools.partial(exchange_kernel, n, groups),
        out_shape=(pltpu.VMEM((tokens, width), BF16), pltpu.VMEM((cols, tokens), BF16), part, part, part),
        in_specs=[hbm] * 3,
        out_specs=(vmem,) * 5,
        scratch_shapes=[
            pltpu.VMEM((cols, width), BF16),
            pltpu.VMEM((tokens, cols), BF16),
            pltpu.VMEM((nb, 2, chips, rows, width // nb), F32),
            pltpu.VMEM((nb, chips, rows, width // nb), F32),
            pltpu.VMEM((nb, rows, width // nb), F32),
            pltpu.VMEM((nb, rows, width // nb), F32),
            pltpu.SemaphoreType.DMA,
            pltpu.SemaphoreType.DMA,
            pltpu.SemaphoreType.DMA((nb,)),
            pltpu.SemaphoreType.DMA((4,)),
            pltpu.SemaphoreType.DMA((4,)),
            pltpu.SemaphoreType.DMA((5,)),
            pltpu.SemaphoreType.DMA((5,)),
            pltpu.SemaphoreType.DMA((nb,)),
            pltpu.SemaphoreType.DMA((nb,)),
            pltpu.SemaphoreType.DMA((2, len(groups))),
            pltpu.SemaphoreType.DMA((2, len(groups))),
        ],
        compiler_params=pltpu.CompilerParams(collective_id=0, has_side_effects=True, vmem_limit_bytes=32 * 2**20),
        cost_estimate=pl.CostEstimate(flops=2 * tokens * width * cols, bytes_accessed=2 * width * cols,
                                      transcendentals=0),
        name="exchange",
    )(*(pltpu.with_memory_space_constraint(a, pltpu.HBM) for a in (x_blk, wt_blk, gt_blk)))


def weight_kernel(x, gt, o_hbm, obuf, o_sem):
    cols, width = o_hbm.shape
    blk = 256
    pieces = [(0, blk, c, min(512, width - c)) for c in range(0, width, 512)]
    pieces += [(r, min(blk, cols - r), 0, width) for r in range(blk, cols, blk)]
    stores = []
    for i, (r, nr, c, nc) in enumerate(pieces):
        rs, cs = pl.ds(r, nr), pl.ds(c, nc)
        obuf[rs, cs] = jnp.dot(gt[rs, :], x[:, cs], preferred_element_type=F32)
        cp = pltpu.make_async_copy(obuf.at[rs, cs], o_hbm.at[rs, cs], o_sem.at[i])
        cp.start()
        stores.append(cp)
    for cp in stores:
        cp.wait()


def weight_grad(x_full, gt_blk):
    tokens, width = x_full.shape
    cols = gt_blk.shape[0]
    vmem = pl.BlockSpec(memory_space=pltpu.VMEM)
    return pl.pallas_call(
        weight_kernel,
        out_shape=jax.ShapeDtypeStruct((cols, width), F32),
        in_specs=[vmem] * 2,
        out_specs=pl.BlockSpec(memory_space=pltpu.HBM),
        scratch_shapes=[pltpu.VMEM((cols, width), F32), pltpu.SemaphoreType.DMA((pl.cdiv(width, 512) + pl.cdiv(cols, 256),))],
        compiler_params=pltpu.CompilerParams(vmem_limit_bytes=40 * 2**20),
        cost_estimate=pl.CostEstimate(flops=2 * tokens * width * cols, bytes_accessed=4 * width * cols,
                                      transcendentals=0),
        name="weight_grad",
    )(x_full, gt_blk)


def solution(mesh):
    n = mesh.shape["tp"]

    def per_device(x_blk, w_blk, grad_blk):
        x_full, gt_blk, own, first, second = exchange(x_blk, w_blk.T, grad_blk.T, n)

        def swap(part, start):
            pairs = []
            for c in range(start, start + n // 2, 2):
                for core in range(2):
                    a, b = (2 * c + core) % n, (2 * c + 2 + core) % n
                    pairs += [(a, b), (b, a)]
            return lax.ppermute(part, "tp", pairs)

        got_first = swap(first, 1)
        got_second = swap(second, 0)
        grad_w = weight_grad(x_full, gt_blk).T
        grad_x = (own + got_first + got_second).astype(BF16)
        return grad_x, grad_w

    return jax.shard_map(
        per_device,
        mesh=mesh,
        in_specs=(P(("dp", "tp"), None), P(None, "tp"), P("dp", "tp")),
        out_specs=(P(("dp", "tp"), None), P("dp", "tp")),
        check_vma=False,
    )
```

```python
import functools

import jax
import jax.numpy as jnp
from jax import lax
from jax.experimental import pallas as pl
from jax.experimental.pallas import tpu as pltpu
from jax.sharding import PartitionSpec as P

MESH = pl.DeviceIdType.MESH
F32 = jnp.float32
BF16 = jnp.bfloat16


def exchange_kernel(n, groups, x_hbm, wt_hbm, gt_hbm, xf, gt, own, first, second,
                    wbuf, g, part, rbuf, opp_sum, u1buf,
                    x_sem, g_sem, w_sem, ag_send, ag_recv, pr_send, pr_recv,
                    d_send, d_recv, u_send, u_recv):
    rows, width = x_hbm.shape
    half = rows // 2
    nb = w_sem.shape[0]
    blk = width // nb
    me = lax.axis_index("tp")
    chips = n // 2
    chip, core = me // 2, lax.rem(me, 2)
    c_right, c_left = lax.rem(chip + 1, chips), lax.rem(chip + chips - 1, chips)
    c_opp = lax.rem(chip + 2, chips)
    right, left, opp = 2 * c_right + core, 2 * c_left + core, 2 * c_opp + core
    peer = 2 * chip + 1 - core
    lo, hi = pl.ds(0, half), pl.ds(half, half)
    odd = lax.rem(chip, 2)
    c_first = odd * c_right + (1 - odd) * c_left
    c_second = odd * c_left + (1 - odd) * c_right
    r_first = pl.multiple_of((1 - odd) * half, half)
    r_second = pl.multiple_of(odd * half, half)

    def at(dev, part_of=0, size=rows):
        return xf.at[pl.ds(pl.multiple_of(dev * rows + part_of * half, half), size), :]

    def low(dev):
        return at(dev, 0, half)

    def high(dev):
        return at(dev, 1, half)

    barrier = pltpu.get_barrier_semaphore()
    for dev in (left, right, peer):
        pl.semaphore_signal(barrier, inc=1, device_id={"tp": dev}, device_id_type=MESH)

    own_x = pltpu.make_async_copy(x_hbm, at(me), x_sem)
    own_x.start()
    g_load = pltpu.make_async_copy(gt_hbm, gt, g_sem)
    g_load.start()
    ahead = 3

    def w_load(j):
        cols = pl.ds(j * blk, blk)
        return pltpu.make_async_copy(wt_hbm.at[:, cols], wbuf.at[:, cols], w_sem.at[j])

    for j in range(ahead):
        w_load(j).start()

    pl.semaphore_wait(barrier, 3)

    def send(src, dst, s_sem, r_sem, dev):
        cp = pltpu.make_async_remote_copy(src_ref=src, dst_ref=dst, send_sem=s_sem, recv_sem=r_sem,
                                          device_id={"tp": dev}, device_id_type=MESH)
        cp.start()
        return cp

    own_x.wait()
    ag = {}
    ag[0] = send(at(me), at(me), ag_send.at[0], ag_recv.at[0], right)
    ag[1] = send(at(me), at(me), ag_send.at[1], ag_recv.at[1], left)
    pr = {}
    pr[4] = send(at(me), at(me), pr_send.at[4], pr_recv.at[4], peer)

    def arrived(slot, block, onward=None):
        pltpu.make_async_remote_copy(src_ref=block, dst_ref=block, send_sem=ag_send.at[slot],
                                     recv_sem=ag_recv.at[slot], device_id={"tp": me}, device_id_type=MESH).wait_recv()
        if onward is not None:
            to, piece, dev = onward
            ag[to] = send(piece, piece, ag_send.at[to], ag_recv.at[to], dev)
        pr[slot] = send(block, block, pr_send.at[slot], pr_recv.at[slot], peer)

    g_load.wait()
    g[...] = gt[...].T

    d2d = {}

    def partial(j):
        w_load(j).wait()
        if j + ahead < nb:
            w_load(j + ahead).start()
        cols = pl.ds(j * blk, blk)
        t = jnp.dot(g[...], wbuf[:, cols], preferred_element_type=F32)
        t = t.reshape(chips, 2, rows, blk)
        for c in range(2):
            part[j, c] = t[:, c]
        d2d[j] = send(part.at[j, 1 - core], rbuf.at[j], d_send.at[j], d_recv.at[j], peer)

    u1 = []

    def chip_sum(js):
        for j in js:
            cols = pl.ds(j * blk, blk)
            d2d[j].wait_recv()
            opp_sum[j] = part[j, core, c_opp] + rbuf[j, c_opp]
            own[:, cols] = part[j, core, chip] + rbuf[j, chip]
            first[:, cols] = part[j, core, c_first] + rbuf[j, c_first]
            second[:, cols] = part[j, core, c_second] + rbuf[j, c_second]
        g0 = pl.ds(js[0], len(js))
        k = len(u1)
        u1.append((js, send(opp_sum.at[g0, lo], u1buf.at[g0, lo], u_send.at[0, k], u_recv.at[0, k], right),
                   send(opp_sum.at[g0, hi], u1buf.at[g0, hi], u_send.at[1, k], u_recv.at[1, k], left)))

    partial(0)
    partial(1)
    partial(2)
    chip_sum(groups[0])
    partial(3)
    partial(4)
    chip_sum(groups[1])
    partial(5)
    partial(6)
    arrived(0, at(left), (2, low(left), right))
    arrived(1, at(right), (3, high(right), left))
    chip_sum(groups[2])
    arrived(2, low(opp))
    arrived(3, high(opp))
    for cp in pr.values():
        cp.wait()
    for cp in ag.values():
        cp.wait_send()
    for cp in d2d.values():
        cp.wait_send()
    for _, a, b in u1:
        a.wait_send()
        b.wait_send()
    for js, from_left, from_right in u1:
        from_left.wait_recv()
        from_right.wait_recv()
        for j in js:
            cols = pl.ds(j * blk, blk)
            first[pl.ds(r_first, half), cols] += u1buf[j, pl.ds(r_first, half)]
            second[pl.ds(r_second, half), cols] += u1buf[j, pl.ds(r_second, half)]


def exchange(x_blk, wt_blk, gt_blk, n):
    rows, width = x_blk.shape
    cols, tokens = gt_blk.shape
    chips = n // 2
    nb = 7
    groups = ((0, 1), (2, 3), (4, 5, 6))
    hbm = pl.BlockSpec(memory_space=pltpu.HBM)
    vmem = pl.BlockSpec(memory_space=pltpu.VMEM)
    part = pltpu.VMEM((rows, width), F32)
    return pl.pallas_call(
        functools.partial(exchange_kernel, n, groups),
        out_shape=(pltpu.VMEM((tokens, width), BF16), pltpu.VMEM((cols, tokens), BF16), part, part, part),
        in_specs=[hbm] * 3,
        out_specs=(vmem,) * 5,
        scratch_shapes=[
            pltpu.VMEM((cols, width), BF16),
            pltpu.VMEM((tokens, cols), BF16),
            pltpu.VMEM((nb, 2, chips, rows, width // nb), F32),
            pltpu.VMEM((nb, chips, rows, width // nb), F32),
            pltpu.VMEM((nb, rows, width // nb), F32),
            pltpu.VMEM((nb, rows, width // nb), F32),
            pltpu.SemaphoreType.DMA,
            pltpu.SemaphoreType.DMA,
            pltpu.SemaphoreType.DMA((nb,)),
            pltpu.SemaphoreType.DMA((4,)),
            pltpu.SemaphoreType.DMA((4,)),
            pltpu.SemaphoreType.DMA((5,)),
            pltpu.SemaphoreType.DMA((5,)),
            pltpu.SemaphoreType.DMA((nb,)),
            pltpu.SemaphoreType.DMA((nb,)),
            pltpu.SemaphoreType.DMA((2, len(groups))),
            pltpu.SemaphoreType.DMA((2, len(groups))),
        ],
        compiler_params=pltpu.CompilerParams(collective_id=0, has_side_effects=True, vmem_limit_bytes=32 * 2**20),
        cost_estimate=pl.CostEstimate(flops=2 * tokens * width * cols, bytes_accessed=2 * width * cols,
                                      transcendentals=0),
        name="exchange",
    )(*(pltpu.with_memory_space_constraint(a, pltpu.HBM) for a in (x_blk, wt_blk, gt_blk)))


def weight_kernel(x, gt, o_hbm, obuf, o_sem):
    cols, width = o_hbm.shape
    blk = 256
    pieces = [(0, blk, c, min(512, width - c)) for c in range(0, width, 512)]
    pieces += [(r, min(blk, cols - r), 0, width) for r in range(blk, cols, blk)]
    stores = []
    for i, (r, nr, c, nc) in enumerate(pieces):
        rs, cs = pl.ds(r, nr), pl.ds(c, nc)
        obuf[rs, cs] = jnp.dot(gt[rs, :], x[:, cs], preferred_element_type=F32)
        cp = pltpu.make_async_copy(obuf.at[rs, cs], o_hbm.at[rs, cs], o_sem.at[i])
        cp.start()
        stores.append(cp)
    for cp in stores:
        cp.wait()


def weight_grad(x_full, gt_blk):
    tokens, width = x_full.shape
    cols = gt_blk.shape[0]
    vmem = pl.BlockSpec(memory_space=pltpu.VMEM)
    return pl.pallas_call(
        weight_kernel,
        out_shape=jax.ShapeDtypeStruct((cols, width), F32),
        in_specs=[vmem] * 2,
        out_specs=pl.BlockSpec(memory_space=pltpu.HBM),
        scratch_shapes=[pltpu.VMEM((cols, width), F32), pltpu.SemaphoreType.DMA((pl.cdiv(width, 512) + pl.cdiv(cols, 256),))],
        compiler_params=pltpu.CompilerParams(vmem_limit_bytes=40 * 2**20),
        cost_estimate=pl.CostEstimate(flops=2 * tokens * width * cols, bytes_accessed=4 * width * cols,
                                      transcendentals=0),
        name="weight_grad",
    )(x_full, gt_blk)


def solution(mesh):
    n = mesh.shape["tp"]

    def per_device(x_blk, w_blk, grad_blk):
        x_full, gt_blk, own, first, second = exchange(x_blk, w_blk.T, grad_blk.T, n)

        def swap(part, start):
            pairs = []
            for c in range(start, start + n // 2, 2):
                for core in range(2):
                    a, b = (2 * c + core) % n, (2 * c + 2 + core) % n
                    pairs += [(a, b), (b, a)]
            return lax.ppermute(part, "tp", pairs)

        got_first = swap(first, 1)
        got_second = swap(second, 0)
        grad_w = weight_grad(x_full, gt_blk).T
        grad_x = (own + got_first + got_second).astype(BF16)
        return grad_x, grad_w

    return jax.shard_map(
        per_device,
        mesh=mesh,
        in_specs=(P(("dp", "tp"), None), P(None, "tp"), P("dp", "tp")),
        out_specs=(P(("dp", "tp"), None), P("dp", "tp")),
        check_vma=False,
    )
```

```python
import functools

import jax
import jax.numpy as jnp
from jax import lax
from jax.experimental import pallas as pl
from jax.experimental.pallas import tpu as pltpu
from jax.sharding import PartitionSpec as P

MESH = pl.DeviceIdType.MESH
F32 = jnp.float32
BF16 = jnp.bfloat16


def exchange_kernel(n, groups, x_hbm, wt_hbm, gt_hbm, xf, gt, own, first, second,
                    wbuf, g, part, rbuf, opp_sum, u1buf,
                    x_sem, g_sem, w_sem, ag_send, ag_recv, pr_send, pr_recv,
                    d_send, d_recv, u_send, u_recv):
    rows, width = x_hbm.shape
    half = rows // 2
    nb = w_sem.shape[0]
    blk = width // nb
    me = lax.axis_index("tp")
    chips = n // 2
    chip, core = me // 2, lax.rem(me, 2)
    c_right, c_left = lax.rem(chip + 1, chips), lax.rem(chip + chips - 1, chips)
    c_opp = lax.rem(chip + 2, chips)
    right, left, opp = 2 * c_right + core, 2 * c_left + core, 2 * c_opp + core
    peer = 2 * chip + 1 - core
    lo, hi = pl.ds(0, half), pl.ds(half, half)
    odd = lax.rem(chip, 2)
    c_first = odd * c_right + (1 - odd) * c_left
    c_second = odd * c_left + (1 - odd) * c_right
    r_first = pl.multiple_of((1 - odd) * half, half)
    r_second = pl.multiple_of(odd * half, half)

    def at(dev, part_of=0, size=rows):
        return xf.at[pl.ds(pl.multiple_of(dev * rows + part_of * half, half), size), :]

    def low(dev):
        return at(dev, 0, half)

    def high(dev):
        return at(dev, 1, half)

    barrier = pltpu.get_barrier_semaphore()
    for dev in (left, right, peer):
        pl.semaphore_signal(barrier, inc=1, device_id={"tp": dev}, device_id_type=MESH)

    own_x = pltpu.make_async_copy(x_hbm, at(me), x_sem)
    own_x.start()
    g_load = pltpu.make_async_copy(gt_hbm, gt, g_sem)
    g_load.start()
    ahead = 3

    def w_load(j):
        cols = pl.ds(j * blk, blk)
        return pltpu.make_async_copy(wt_hbm.at[:, cols], wbuf.at[:, cols], w_sem.at[j])

    for j in range(ahead):
        w_load(j).start()

    pl.semaphore_wait(barrier, 3)

    def send(src, dst, s_sem, r_sem, dev):
        cp = pltpu.make_async_remote_copy(src_ref=src, dst_ref=dst, send_sem=s_sem, recv_sem=r_sem,
                                          device_id={"tp": dev}, device_id_type=MESH)
        cp.start()
        return cp

    own_x.wait()
    ag = {}
    ag[0] = send(low(me), low(me), ag_send.at[0], ag_recv.at[0], right)
    ag[3] = send(high(me), high(me), ag_send.at[3], ag_recv.at[3], left)
    ag[1] = send(high(me), high(me), ag_send.at[1], ag_recv.at[1], right)
    ag[2] = send(low(me), low(me), ag_send.at[2], ag_recv.at[2], left)
    pr = {}
    pr[6] = send(at(me), at(me), pr_send.at[6], pr_recv.at[6], peer)

    def arrived(slot, block, onward=None):
        pltpu.make_async_remote_copy(src_ref=block, dst_ref=block, send_sem=ag_send.at[slot],
                                     recv_sem=ag_recv.at[slot], device_id={"tp": me}, device_id_type=MESH).wait_recv()
        if onward is not None:
            to, dev = onward
            ag[to] = send(block, block, ag_send.at[to], ag_recv.at[to], dev)
        pr[slot] = send(block, block, pr_send.at[slot], pr_recv.at[slot], peer)

    g_load.wait()
    g[...] = gt[...].T

    d2d = {}

    def partial(j):
        w_load(j).wait()
        if j + ahead < nb:
            w_load(j + ahead).start()
        cols = pl.ds(j * blk, blk)
        t = jnp.dot(g[...], wbuf[:, cols], preferred_element_type=F32)
        t = t.reshape(chips, 2, rows, blk)
        for c in range(2):
            part[j, c] = t[:, c]
        d2d[j] = send(part.at[j, 1 - core], rbuf.at[j], d_send.at[j], d_recv.at[j], peer)

    u1 = []

    def chip_sum(js):
        for j in js:
            cols = pl.ds(j * blk, blk)
            d2d[j].wait_recv()
            opp_sum[j] = part[j, core, c_opp] + rbuf[j, c_opp]
            own[:, cols] = part[j, core, chip] + rbuf[j, chip]
            first[:, cols] = part[j, core, c_first] + rbuf[j, c_first]
            second[:, cols] = part[j, core, c_second] + rbuf[j, c_second]
        g0 = pl.ds(js[0], len(js))
        k = len(u1)
        u1.append((js, send(opp_sum.at[g0, lo], u1buf.at[g0, lo], u_send.at[0, k], u_recv.at[0, k], right),
                   send(opp_sum.at[g0, hi], u1buf.at[g0, hi], u_send.at[1, k], u_recv.at[1, k], left)))

    partial(0)
    partial(1)
    partial(2)
    chip_sum(groups[0])
    partial(3)
    arrived(0, low(left), (4, right))
    arrived(3, high(right), (5, left))
    partial(4)
    chip_sum(groups[1])
    partial(5)
    partial(6)
    arrived(1, high(left))
    arrived(2, low(right))
    chip_sum(groups[2])
    arrived(4, low(opp))
    arrived(5, high(opp))
    for cp in pr.values():
        cp.wait()
    for cp in ag.values():
        cp.wait_send()
    for cp in d2d.values():
        cp.wait_send()
    for _, a, b in u1:
        a.wait_send()
        b.wait_send()
    for js, from_left, from_right in u1:
        from_left.wait_recv()
        from_right.wait_recv()
        for j in js:
            cols = pl.ds(j * blk, blk)
            first[pl.ds(r_first, half), cols] += u1buf[j, pl.ds(r_first, half)]
            second[pl.ds(r_second, half), cols] += u1buf[j, pl.ds(r_second, half)]


def exchange(x_blk, wt_blk, gt_blk, n):
    rows, width = x_blk.shape
    cols, tokens = gt_blk.shape
    chips = n // 2
    nb = 7
    groups = ((0, 1), (2, 3), (4, 5, 6))
    hbm = pl.BlockSpec(memory_space=pltpu.HBM)
    vmem = pl.BlockSpec(memory_space=pltpu.VMEM)
    part = pltpu.VMEM((rows, width), F32)
    return pl.pallas_call(
        functools.partial(exchange_kernel, n, groups),
        out_shape=(pltpu.VMEM((tokens, width), BF16), pltpu.VMEM((cols, tokens), BF16), part, part, part),
        in_specs=[hbm] * 3,
        out_specs=(vmem,) * 5,
        scratch_shapes=[
            pltpu.VMEM((cols, width), BF16),
            pltpu.VMEM((tokens, cols), BF16),
            pltpu.VMEM((nb, 2, chips, rows, width // nb), F32),
            pltpu.VMEM((nb, chips, rows, width // nb), F32),
            pltpu.VMEM((nb, rows, width // nb), F32),
            pltpu.VMEM((nb, rows, width // nb), F32),
            pltpu.SemaphoreType.DMA,
            pltpu.SemaphoreType.DMA,
            pltpu.SemaphoreType.DMA((nb,)),
            pltpu.SemaphoreType.DMA((6,)),
            pltpu.SemaphoreType.DMA((6,)),
            pltpu.SemaphoreType.DMA((7,)),
            pltpu.SemaphoreType.DMA((7,)),
            pltpu.SemaphoreType.DMA((nb,)),
            pltpu.SemaphoreType.DMA((nb,)),
            pltpu.SemaphoreType.DMA((2, len(groups))),
            pltpu.SemaphoreType.DMA((2, len(groups))),
        ],
        compiler_params=pltpu.CompilerParams(collective_id=0, has_side_effects=True, vmem_limit_bytes=32 * 2**20),
        cost_estimate=pl.CostEstimate(flops=2 * tokens * width * cols, bytes_accessed=2 * width * cols,
                                      transcendentals=0),
        name="exchange",
    )(*(pltpu.with_memory_space_constraint(a, pltpu.HBM) for a in (x_blk, wt_blk, gt_blk)))


def weight_kernel(x, gt, o_hbm, obuf, o_sem):
    cols, width = o_hbm.shape
    blk = 256
    pieces = [(0, blk, c, min(512, width - c)) for c in range(0, width, 512)]
    pieces += [(r, min(blk, cols - r), 0, width) for r in range(blk, cols, blk)]
    stores = []
    for i, (r, nr, c, nc) in enumerate(pieces):
        rs, cs = pl.ds(r, nr), pl.ds(c, nc)
        obuf[rs, cs] = jnp.dot(gt[rs, :], x[:, cs], preferred_element_type=F32)
        cp = pltpu.make_async_copy(obuf.at[rs, cs], o_hbm.at[rs, cs], o_sem.at[i])
        cp.start()
        stores.append(cp)
    for cp in stores:
        cp.wait()


def weight_grad(x_full, gt_blk):
    tokens, width = x_full.shape
    cols = gt_blk.shape[0]
    vmem = pl.BlockSpec(memory_space=pltpu.VMEM)
    return pl.pallas_call(
        weight_kernel,
        out_shape=jax.ShapeDtypeStruct((cols, width), F32),
        in_specs=[vmem] * 2,
        out_specs=pl.BlockSpec(memory_space=pltpu.HBM),
        scratch_shapes=[pltpu.VMEM((cols, width), F32), pltpu.SemaphoreType.DMA((pl.cdiv(width, 512) + pl.cdiv(cols, 256),))],
        compiler_params=pltpu.CompilerParams(vmem_limit_bytes=40 * 2**20),
        cost_estimate=pl.CostEstimate(flops=2 * tokens * width * cols, bytes_accessed=4 * width * cols,
                                      transcendentals=0),
        name="weight_grad",
    )(x_full, gt_blk)


def solution(mesh):
    n = mesh.shape["tp"]

    def per_device(x_blk, w_blk, grad_blk):
        x_full, gt_blk, own, first, second = exchange(x_blk, w_blk.T, grad_blk.T, n)

        def swap(part, start):
            pairs = []
            for c in range(start, start + n // 2, 2):
                for core in range(2):
                    a, b = (2 * c + core) % n, (2 * c + 2 + core) % n
                    pairs += [(a, b), (b, a)]
            return lax.ppermute(part, "tp", pairs)

        got_first = swap(first, 1)
        got_second = swap(second, 0)
        grad_w = weight_grad(x_full, gt_blk).T
        grad_x = (own + got_first + got_second).astype(BF16)
        return grad_x, grad_w

    return jax.shard_map(
        per_device,
        mesh=mesh,
        in_specs=(P(("dp", "tp"), None), P(None, "tp"), P("dp", "tp")),
        out_specs=(P(("dp", "tp"), None), P("dp", "tp")),
        check_vma=False,
    )
```

```python
import functools

import jax
import jax.numpy as jnp
from jax import lax
from jax.experimental import pallas as pl
from jax.experimental.pallas import tpu as pltpu
from jax.sharding import PartitionSpec as P

MESH = pl.DeviceIdType.MESH
F32 = jnp.float32
BF16 = jnp.bfloat16


def exchange_kernel(n, groups, x_hbm, wt_hbm, gt_hbm, xf, gt, own, first, second,
                    wbuf, g, part, rbuf, opp_sum, u1buf,
                    x_sem, g_sem, w_sem, ag_send, ag_recv, pr_send, pr_recv,
                    d_send, d_recv, u_send, u_recv):
    rows, width = x_hbm.shape
    half = rows // 2
    nb = w_sem.shape[0]
    blk = width // nb
    me = lax.axis_index("tp")
    chips = n // 2
    chip, core = me // 2, lax.rem(me, 2)
    c_right, c_left = lax.rem(chip + 1, chips), lax.rem(chip + chips - 1, chips)
    c_opp = lax.rem(chip + 2, chips)
    right, left, opp = 2 * c_right + core, 2 * c_left + core, 2 * c_opp + core
    peer = 2 * chip + 1 - core
    lo, hi = pl.ds(0, half), pl.ds(half, half)
    odd = lax.rem(chip, 2)
    c_first = odd * c_right + (1 - odd) * c_left
    c_second = odd * c_left + (1 - odd) * c_right
    r_first = pl.multiple_of((1 - odd) * half, half)
    r_second = pl.multiple_of(odd * half, half)

    def at(dev, part_of=0, size=rows):
        return xf.at[pl.ds(pl.multiple_of(dev * rows + part_of * half, half), size), :]

    def low(dev):
        return at(dev, 0, half)

    def high(dev):
        return at(dev, 1, half)

    barrier = pltpu.get_barrier_semaphore()
    for dev in (left, right, peer):
        pl.semaphore_signal(barrier, inc=1, device_id={"tp": dev}, device_id_type=MESH)

    own_x = pltpu.make_async_copy(x_hbm, at(me), x_sem)
    own_x.start()
    g_load = pltpu.make_async_copy(gt_hbm, gt, g_sem)
    g_load.start()
    ahead = 3

    def w_load(j):
        cols = pl.ds(j * blk, blk)
        return pltpu.make_async_copy(wt_hbm.at[:, cols], wbuf.at[:, cols], w_sem.at[j])

    for j in range(ahead):
        w_load(j).start()

    pl.semaphore_wait(barrier, 3)

    def send(src, dst, s_sem, r_sem, dev):
        cp = pltpu.make_async_remote_copy(src_ref=src, dst_ref=dst, send_sem=s_sem, recv_sem=r_sem,
                                          device_id={"tp": dev}, device_id_type=MESH)
        cp.start()
        return cp

    own_x.wait()
    ag = {}
    ag[0] = send(low(me), low(me), ag_send.at[0], ag_recv.at[0], right)
    ag[3] = send(high(me), high(me), ag_send.at[3], ag_recv.at[3], left)
    ag[1] = send(high(me), high(me), ag_send.at[1], ag_recv.at[1], right)
    ag[2] = send(low(me), low(me), ag_send.at[2], ag_recv.at[2], left)
    pr = {}
    pr[6] = send(at(me), at(me), pr_send.at[6], pr_recv.at[6], peer)

    def arrived(slot, block, onward=None):
        pltpu.make_async_remote_copy(src_ref=block, dst_ref=block, send_sem=ag_send.at[slot],
                                     recv_sem=ag_recv.at[slot], device_id={"tp": me}, device_id_type=MESH).wait_recv()
        if onward is not None:
            to, dev = onward
            ag[to] = send(block, block, ag_send.at[to], ag_recv.at[to], dev)
        pr[slot] = send(block, block, pr_send.at[slot], pr_recv.at[slot], peer)

    g_load.wait()
    g[...] = gt[...].T

    d2d = {}

    def partial(j):
        w_load(j).wait()
        if j + ahead < nb:
            w_load(j + ahead).start()
        cols = pl.ds(j * blk, blk)
        t = jnp.dot(g[...], wbuf[:, cols], preferred_element_type=F32)
        t = t.reshape(chips, 2, rows, blk)
        for c in range(2):
            part[j, c] = t[:, c]
        d2d[j] = send(part.at[j, 1 - core], rbuf.at[j], d_send.at[j], d_recv.at[j], peer)

    def chip_sum(js):
        for j in js:
            cols = pl.ds(j * blk, blk)
            d2d[j].wait_recv()
            opp_sum[j] = part[j, core, c_opp] + rbuf[j, c_opp]
            own[:, cols] = part[j, core, chip] + rbuf[j, chip]
            first[:, cols] = part[j, core, c_first] + rbuf[j, c_first]
            second[:, cols] = part[j, core, c_second] + rbuf[j, c_second]

    def group(k):
        g0 = pl.ds(groups[k][0], len(groups[k]))
        copies = [pltpu.make_async_remote_copy(src_ref=opp_sum.at[g0, side], dst_ref=u1buf.at[g0, side],
                                               send_sem=u_send.at[i, k], recv_sem=u_recv.at[i, k],
                                               device_id={"tp": dev}, device_id_type=MESH)
                  for i, (side, dev) in enumerate(((lo, right), (hi, left)))]
        return groups[k], *copies

    def send_group(k):
        for cp in group(k)[1:]:
            cp.start()


    partial(0)
    partial(1)
    partial(2)
    chip_sum(groups[0])

    @pl.when(core == 1)
    def _():
        send_group(0)

    partial(3)
    arrived(0, low(left), (4, right))
    arrived(3, high(right), (5, left))

    @pl.when(core == 0)
    def _():
        send_group(0)

    partial(4)
    chip_sum(groups[1])
    send_group(1)
    partial(5)
    partial(6)
    arrived(1, high(left))
    arrived(2, low(right))
    chip_sum(groups[2])
    send_group(2)
    u1 = [group(k) for k in range(len(groups))]
    arrived(4, low(opp))
    arrived(5, high(opp))
    for cp in pr.values():
        cp.wait()
    for cp in ag.values():
        cp.wait_send()
    for cp in d2d.values():
        cp.wait_send()
    for _, a, b in u1:
        a.wait_send()
        b.wait_send()
    for js, from_left, from_right in u1:
        from_left.wait_recv()
        from_right.wait_recv()
        for j in js:
            cols = pl.ds(j * blk, blk)
            first[pl.ds(r_first, half), cols] += u1buf[j, pl.ds(r_first, half)]
            second[pl.ds(r_second, half), cols] += u1buf[j, pl.ds(r_second, half)]


def exchange(x_blk, wt_blk, gt_blk, n):
    rows, width = x_blk.shape
    cols, tokens = gt_blk.shape
    chips = n // 2
    nb = 7
    groups = ((0, 1), (2, 3), (4, 5, 6))
    hbm = pl.BlockSpec(memory_space=pltpu.HBM)
    vmem = pl.BlockSpec(memory_space=pltpu.VMEM)
    part = pltpu.VMEM((rows, width), F32)
    return pl.pallas_call(
        functools.partial(exchange_kernel, n, groups),
        out_shape=(pltpu.VMEM((tokens, width), BF16), pltpu.VMEM((cols, tokens), BF16), part, part, part),
        in_specs=[hbm] * 3,
        out_specs=(vmem,) * 5,
        scratch_shapes=[
            pltpu.VMEM((cols, width), BF16),
            pltpu.VMEM((tokens, cols), BF16),
            pltpu.VMEM((nb, 2, chips, rows, width // nb), F32),
            pltpu.VMEM((nb, chips, rows, width // nb), F32),
            pltpu.VMEM((nb, rows, width // nb), F32),
            pltpu.VMEM((nb, rows, width // nb), F32),
            pltpu.SemaphoreType.DMA,
            pltpu.SemaphoreType.DMA,
            pltpu.SemaphoreType.DMA((nb,)),
            pltpu.SemaphoreType.DMA((6,)),
            pltpu.SemaphoreType.DMA((6,)),
            pltpu.SemaphoreType.DMA((7,)),
            pltpu.SemaphoreType.DMA((7,)),
            pltpu.SemaphoreType.DMA((nb,)),
            pltpu.SemaphoreType.DMA((nb,)),
            pltpu.SemaphoreType.DMA((2, len(groups))),
            pltpu.SemaphoreType.DMA((2, len(groups))),
        ],
        compiler_params=pltpu.CompilerParams(collective_id=0, has_side_effects=True, vmem_limit_bytes=32 * 2**20),
        cost_estimate=pl.CostEstimate(flops=2 * tokens * width * cols, bytes_accessed=2 * width * cols,
                                      transcendentals=0),
        name="exchange",
    )(*(pltpu.with_memory_space_constraint(a, pltpu.HBM) for a in (x_blk, wt_blk, gt_blk)))


def weight_kernel(x, gt, o_hbm, obuf, o_sem):
    cols, width = o_hbm.shape
    blk = 256
    cuts = [width // 7 * c for c in (0, 1, 3, 7)]
    pieces = [(0, blk, a, b - a) for a, b in zip(cuts, cuts[1:])]
    pieces += [(r, min(blk, cols - r), 0, width) for r in range(blk, cols, blk)]
    stores = []
    for i, (r, nr, c, nc) in enumerate(pieces):
        rs, cs = pl.ds(r, nr), pl.ds(c, nc)
        obuf[rs, cs] = jnp.dot(gt[rs, :], x[:, cs], preferred_element_type=F32)
        cp = pltpu.make_async_copy(obuf.at[rs, cs], o_hbm.at[rs, cs], o_sem.at[i])
        cp.start()
        stores.append(cp)
    for cp in stores:
        cp.wait()


def weight_grad(x_full, gt_blk):
    tokens, width = x_full.shape
    cols = gt_blk.shape[0]
    vmem = pl.BlockSpec(memory_space=pltpu.VMEM)
    return pl.pallas_call(
        weight_kernel,
        out_shape=jax.ShapeDtypeStruct((cols, width), F32),
        in_specs=[vmem] * 2,
        out_specs=pl.BlockSpec(memory_space=pltpu.HBM),
        scratch_shapes=[pltpu.VMEM((cols, width), F32), pltpu.SemaphoreType.DMA((pl.cdiv(width, 512) + pl.cdiv(cols, 256),))],
        compiler_params=pltpu.CompilerParams(vmem_limit_bytes=40 * 2**20),
        cost_estimate=pl.CostEstimate(flops=2 * tokens * width * cols, bytes_accessed=4 * width * cols,
                                      transcendentals=0),
        name="weight_grad",
    )(x_full, gt_blk)


def solution(mesh):
    n = mesh.shape["tp"]

    def per_device(x_blk, w_blk, grad_blk):
        x_full, gt_blk, own, first, second = exchange(x_blk, w_blk.T, grad_blk.T, n)

        def swap(part, start):
            pairs = []
            for c in range(start, start + n // 2, 2):
                for core in range(2):
                    a, b = (2 * c + core) % n, (2 * c + 2 + core) % n
                    pairs += [(a, b), (b, a)]
            return lax.ppermute(part, "tp", pairs)

        got_first = swap(first, 1)
        got_second = swap(second, 0)
        grad_w = weight_grad(x_full, gt_blk).T
        grad_x = (own + got_first + got_second).astype(BF16)
        return grad_x, grad_w

    return jax.shard_map(
        per_device,
        mesh=mesh,
        in_specs=(P(("dp", "tp"), None), P(None, "tp"), P("dp", "tp")),
        out_specs=(P(("dp", "tp"), None), P("dp", "tp")),
        check_vma=False,
    )
```

```python
import functools

import jax
import jax.numpy as jnp
from jax import lax
from jax.experimental import pallas as pl
from jax.experimental.pallas import tpu as pltpu
from jax.sharding import PartitionSpec as P

MESH = pl.DeviceIdType.MESH
F32 = jnp.float32
BF16 = jnp.bfloat16


def exchange_kernel(n, groups, x_hbm, wt_hbm, gt_hbm, xf, gt, own, first, second,
                    wbuf, g, part, rbuf, opp_sum, u1buf,
                    x_sem, g_sem, w_sem, ag_send, ag_recv, pr_send, pr_recv,
                    d_send, d_recv, u_send, u_recv):
    rows, width = x_hbm.shape
    half = rows // 2
    nb = w_sem.shape[0]
    blk = width // nb
    me = lax.axis_index("tp")
    chips = n // 2
    chip, core = me // 2, lax.rem(me, 2)
    c_right, c_left = lax.rem(chip + 1, chips), lax.rem(chip + chips - 1, chips)
    c_opp = lax.rem(chip + 2, chips)
    right, left, opp = 2 * c_right + core, 2 * c_left + core, 2 * c_opp + core
    peer = 2 * chip + 1 - core
    lo, hi = pl.ds(0, half), pl.ds(half, half)
    odd = lax.rem(chip, 2)
    c_first = odd * c_right + (1 - odd) * c_left
    c_second = odd * c_left + (1 - odd) * c_right
    r_first = pl.multiple_of((1 - odd) * half, half)
    r_second = pl.multiple_of(odd * half, half)

    def at(dev, part_of=0, size=rows):
        return xf.at[pl.ds(pl.multiple_of(dev * rows + part_of * half, half), size), :]

    def low(dev):
        return at(dev, 0, half)

    def high(dev):
        return at(dev, 1, half)

    barrier = pltpu.get_barrier_semaphore()
    for dev in (left, right, peer):
        pl.semaphore_signal(barrier, inc=1, device_id={"tp": dev}, device_id_type=MESH)

    own_x = pltpu.make_async_copy(x_hbm, at(me), x_sem)
    own_x.start()
    g_load = pltpu.make_async_copy(gt_hbm, gt, g_sem)
    g_load.start()
    ahead = 3

    def w_load(j):
        cols = pl.ds(j * blk, blk)
        return pltpu.make_async_copy(wt_hbm.at[:, cols], wbuf.at[:, cols], w_sem.at[j])

    for j in range(ahead):
        w_load(j).start()

    pl.semaphore_wait(barrier, 3)

    def send(src, dst, s_sem, r_sem, dev):
        cp = pltpu.make_async_remote_copy(src_ref=src, dst_ref=dst, send_sem=s_sem, recv_sem=r_sem,
                                          device_id={"tp": dev}, device_id_type=MESH)
        cp.start()
        return cp

    own_x.wait()
    ag = {}
    ag[0] = send(low(me), low(me), ag_send.at[0], ag_recv.at[0], right)
    ag[3] = send(high(me), high(me), ag_send.at[3], ag_recv.at[3], left)
    ag[1] = send(high(me), high(me), ag_send.at[1], ag_recv.at[1], right)
    ag[2] = send(low(me), low(me), ag_send.at[2], ag_recv.at[2], left)
    pr = {}
    pr[6] = send(at(me), at(me), pr_send.at[6], pr_recv.at[6], peer)

    def arrived(slot, block, onward=None):
        pltpu.make_async_remote_copy(src_ref=block, dst_ref=block, send_sem=ag_send.at[slot],
                                     recv_sem=ag_recv.at[slot], device_id={"tp": me}, device_id_type=MESH).wait_recv()
        if onward is not None:
            to, dev = onward
            ag[to] = send(block, block, ag_send.at[to], ag_recv.at[to], dev)
        pr[slot] = send(block, block, pr_send.at[slot], pr_recv.at[slot], peer)

    g_load.wait()
    g[...] = gt[...].T

    d2d = {}

    def partial(j):
        w_load(j).wait()
        if j + ahead < nb:
            w_load(j + ahead).start()
        cols = pl.ds(j * blk, blk)
        t = jnp.dot(g[...], wbuf[:, cols], preferred_element_type=F32)
        t = t.reshape(chips, 2, rows, blk)
        for c in range(2):
            part[j, c] = t[:, c]
        d2d[j] = send(part.at[j, 1 - core], rbuf.at[j], d_send.at[j], d_recv.at[j], peer)

    u1 = []

    def chip_sum(js):
        for j in js:
            cols = pl.ds(j * blk, blk)
            d2d[j].wait_recv()
            opp_sum[j] = part[j, core, c_opp] + rbuf[j, c_opp]
            own[:, cols] = part[j, core, chip] + rbuf[j, chip]
            first[:, cols] = part[j, core, c_first] + rbuf[j, c_first]
            second[:, cols] = part[j, core, c_second] + rbuf[j, c_second]
        g0 = pl.ds(js[0], len(js))
        k = len(u1)
        u1.append((js, send(opp_sum.at[g0, lo], u1buf.at[g0, lo], u_send.at[0, k], u_recv.at[0, k], right),
                   send(opp_sum.at[g0, hi], u1buf.at[g0, hi], u_send.at[1, k], u_recv.at[1, k], left)))

    partial(0)
    partial(1)
    partial(2)
    chip_sum(groups[0])
    partial(3)
    arrived(0, low(left), (4, right))
    arrived(3, high(right), (5, left))
    partial(4)
    chip_sum(groups[1])
    partial(5)
    partial(6)
    arrived(1, high(left))
    arrived(2, low(right))
    chip_sum(groups[2])

    def finish(entry):
        js, from_left, from_right = entry
        from_left.wait_recv()
        from_right.wait_recv()
        for j in js:
            cols = pl.ds(j * blk, blk)
            first[pl.ds(r_first, half), cols] += u1buf[j, pl.ds(r_first, half)]
            second[pl.ds(r_second, half), cols] += u1buf[j, pl.ds(r_second, half)]

    finish(u1[0])
    arrived(4, low(opp))
    arrived(5, high(opp))
    finish(u1[1])
    for cp in pr.values():
        cp.wait()
    for cp in ag.values():
        cp.wait_send()
    for cp in d2d.values():
        cp.wait_send()
    for _, a, b in u1:
        a.wait_send()
        b.wait_send()
    finish(u1[2])


def exchange(x_blk, wt_blk, gt_blk, n):
    rows, width = x_blk.shape
    cols, tokens = gt_blk.shape
    chips = n // 2
    nb = 7
    groups = ((0, 1), (2, 3), (4, 5, 6))
    hbm = pl.BlockSpec(memory_space=pltpu.HBM)
    vmem = pl.BlockSpec(memory_space=pltpu.VMEM)
    part = pltpu.VMEM((rows, width), F32)
    return pl.pallas_call(
        functools.partial(exchange_kernel, n, groups),
        out_shape=(pltpu.VMEM((tokens, width), BF16), pltpu.VMEM((cols, tokens), BF16), part, part, part),
        in_specs=[hbm] * 3,
        out_specs=(vmem,) * 5,
        scratch_shapes=[
            pltpu.VMEM((cols, width), BF16),
            pltpu.VMEM((tokens, cols), BF16),
            pltpu.VMEM((nb, 2, chips, rows, width // nb), F32),
            pltpu.VMEM((nb, chips, rows, width // nb), F32),
            pltpu.VMEM((nb, rows, width // nb), F32),
            pltpu.VMEM((nb, rows, width // nb), F32),
            pltpu.SemaphoreType.DMA,
            pltpu.SemaphoreType.DMA,
            pltpu.SemaphoreType.DMA((nb,)),
            pltpu.SemaphoreType.DMA((6,)),
            pltpu.SemaphoreType.DMA((6,)),
            pltpu.SemaphoreType.DMA((7,)),
            pltpu.SemaphoreType.DMA((7,)),
            pltpu.SemaphoreType.DMA((nb,)),
            pltpu.SemaphoreType.DMA((nb,)),
            pltpu.SemaphoreType.DMA((2, len(groups))),
            pltpu.SemaphoreType.DMA((2, len(groups))),
        ],
        compiler_params=pltpu.CompilerParams(collective_id=0, has_side_effects=True, vmem_limit_bytes=32 * 2**20),
        cost_estimate=pl.CostEstimate(flops=2 * tokens * width * cols, bytes_accessed=2 * width * cols,
                                      transcendentals=0),
        name="exchange",
    )(*(pltpu.with_memory_space_constraint(a, pltpu.HBM) for a in (x_blk, wt_blk, gt_blk)))


def weight_kernel(x, gt, o_hbm, obuf, o_sem):
    cols, width = o_hbm.shape
    blk = 256
    pieces = [(0, blk, c, min(512, width - c)) for c in range(0, width, 512)]
    pieces += [(r, min(blk, cols - r), 0, width) for r in range(blk, cols, blk)]
    stores = []
    for i, (r, nr, c, nc) in enumerate(pieces):
        rs, cs = pl.ds(r, nr), pl.ds(c, nc)
        obuf[rs, cs] = jnp.dot(gt[rs, :], x[:, cs], preferred_element_type=F32)
        cp = pltpu.make_async_copy(obuf.at[rs, cs], o_hbm.at[rs, cs], o_sem.at[i])
        cp.start()
        stores.append(cp)
    for cp in stores:
        cp.wait()


def weight_grad(x_full, gt_blk):
    tokens, width = x_full.shape
    cols = gt_blk.shape[0]
    vmem = pl.BlockSpec(memory_space=pltpu.VMEM)
    return pl.pallas_call(
        weight_kernel,
        out_shape=jax.ShapeDtypeStruct((cols, width), F32),
        in_specs=[vmem] * 2,
        out_specs=pl.BlockSpec(memory_space=pltpu.HBM),
        scratch_shapes=[pltpu.VMEM((cols, width), F32), pltpu.SemaphoreType.DMA((pl.cdiv(width, 512) + pl.cdiv(cols, 256),))],
        compiler_params=pltpu.CompilerParams(vmem_limit_bytes=40 * 2**20),
        cost_estimate=pl.CostEstimate(flops=2 * tokens * width * cols, bytes_accessed=4 * width * cols,
                                      transcendentals=0),
        name="weight_grad",
    )(x_full, gt_blk)


def solution(mesh):
    n = mesh.shape["tp"]

    def per_device(x_blk, w_blk, grad_blk):
        x_full, gt_blk, own, first, second = exchange(x_blk, w_blk.T, grad_blk.T, n)

        def swap(part, start):
            pairs = []
            for c in range(start, start + n // 2, 2):
                for core in range(2):
                    a, b = (2 * c + core) % n, (2 * c + 2 + core) % n
                    pairs += [(a, b), (b, a)]
            return lax.ppermute(part, "tp", pairs)

        got_first = swap(first, 1)
        got_second = swap(second, 0)
        grad_w = weight_grad(x_full, gt_blk).T
        grad_x = (own + got_first + got_second).astype(BF16)
        return grad_x, grad_w

    return jax.shard_map(
        per_device,
        mesh=mesh,
        in_specs=(P(("dp", "tp"), None), P(None, "tp"), P("dp", "tp")),
        out_specs=(P(("dp", "tp"), None), P("dp", "tp")),
        check_vma=False,
    )
```
